32 devices in a mesh: leaf: 4 (over y, x), blk: 8 (over z, core).
Axes of the slice: x: 2, y: 2, z: 4, core: 2. Of those that a mesh axis runs over, the one named last changes fastest.
Arguments:
- leaf_rhs: bfloat16 [10240, 256], P(('leaf', 'blk')), may hold values from -6 to 6
- leaf_inverse: bfloat16 [10240, 2560], P(('leaf', 'blk')), may hold values from -0.125 to 0.125
- leaf_lower: bfloat16 [4096, 2560], P(('leaf', 'blk')), may hold values from -0.125 to 0.125
- sep_rhs: bfloat16 [2, 2048, 256], P(None, ('leaf', 'blk')), may hold values from -6 to 6
- sep_inverse: bfloat16 [2048, 3072], P(('leaf', 'blk'))
- sep_lower: bfloat16 [4096, 1024], P(('leaf', 'blk'))
- slot_map: int32 [2, 32, 2], P(None, ('leaf', 'blk')), may hold values from 0 to 5, as said below
Outputs:
- leaf_solution: bfloat16 [10240, 256], P(('leaf', 'blk'))
- sep_solution: bfloat16 [2, 2048, 256], P(None, ('leaf', 'blk'))
The draws below stay inside these ranges and needn't reach their ends.
Inputs may be any that keep to these rules, and one draw needn't show every extreme that they name: For every level below the top, slot_map[h-1, q] holds two different numbers of 0 to 5; at the top level it holds 0 and 1 in some order.
All inputs are finite; a program needn't handle non-finite values.
Results may differ from the reference program's by a relative error of at most 0.015.
Values may be sent and summed in bfloat16 or wider, within the bound.
No kernel may reach another device: no remote copies, remote signals or barrier semaphores. Data moves between devices by JAX's collectives and lax.ppermute only.
A program may use at most 128 MiB of HBM per device.

```python
import jax
import jax.numpy as jnp
from jax import lax

RHS = 256
PIV_DEV = 64
UPD_DEV = 128
LV = 2
POS = 32
SN0 = 2560
SEP_UNIT = 512
SEP_COLS = 3072
LOW_COLS = 1024
LEAF_ROWS = 10240
LOW_ROWS = 4096
SEP_ROWS = 2048
N_LEAF = 4
N_BLK = 8


def column_scale(columns_total):
    col_index = jnp.arange(columns_total, dtype=jnp.int32)
    height = jnp.zeros((columns_total,), jnp.float32)
    for step_index in range(1, LV + 1):
        height = height + (col_index >= SEP_UNIT * (2 ** step_index - 2)).astype(jnp.float32)
    return jax.lax.rsqrt(SEP_UNIT * jnp.exp2(height))


def scaled_block(key, row_count, columns_total):
    values = jax.random.normal(key, (row_count, columns_total), jnp.float32)
    return (values * column_scale(columns_total)[None, :]).astype(jnp.bfloat16)


def draw_sep_inverse(key, part):
    return scaled_block(jax.random.fold_in(key, 11), POS * PIV_DEV, SEP_COLS)


def draw_sep_lower(key, part):
    return scaled_block(jax.random.fold_in(key, 13), POS * UPD_DEV, LOW_COLS)


def draw_slot_map(key, part):
    scores = jax.random.randint(jax.random.fold_in(key, 17), (LV, POS, 6), 0, 1 << 26) * 8 + jnp.arange(6, dtype=jnp.int32)
    heights = jnp.arange(LV, dtype=jnp.int32)[:, None, None]
    blocked = (heights == LV - 1) & (jnp.arange(6, dtype=jnp.int32)[None, None, :] >= 2)
    scores = jnp.where(blocked, 1 << 30, scores)
    ordering = jnp.argsort(scores, axis=-1)
    return ordering[:, :, :2].astype(jnp.int32)


def steps_of(stream_key, dims, cuts, least, top_value):
    level = 1.0
    for dim, shards_of in cuts:
        steps = jax.random.uniform(jax.random.fold_in(jax.random.fold_in(stream_key, 6), dim), (shards_of,), jnp.float32, least / len(cuts), top_value / len(cuts))
        level = level * jnp.repeat(jnp.exp(steps), dims[dim] // shards_of).reshape((-1,) + (1,) * (len(dims) - 1 - dim))
    return level


def bell_draw(stream_key, extent, spread, most, split=(), kind=jnp.bfloat16):
    level = steps_of(stream_key, extent, split, -0.22, 0.18) if split else 1.0
    array = jax.random.normal(stream_key, extent, jnp.float32) * spread * level
    return jnp.minimum(jnp.maximum(array, -most), most).astype(kind)


def setup_inputs(seed: int = 0) -> dict:
    streams_of = jax.random.split(jax.random.key(seed), 8)
    leaf_rhs = bell_draw(streams_of[0], (LEAF_ROWS, RHS), 1.0, 6.0, ((0, 32),))
    leaf_inverse = bell_draw(streams_of[1], (LEAF_ROWS, SN0), SN0 ** -0.5, 0.125, ((0, 32),))
    leaf_lower = bell_draw(streams_of[2], (LOW_ROWS, SN0), SN0 ** -0.5, 0.125, ((0, 32),))
    sep_rhs = bell_draw(streams_of[3], (LV, SEP_ROWS, RHS), 1.0, 6.0, ((1, 32),))
    sep_inverse = draw_sep_inverse(jax.random.fold_in(streams_of[7], 71), 0)
    sep_lower = draw_sep_lower(jax.random.fold_in(streams_of[7], 71), 0)
    slot_map = draw_slot_map(jax.random.fold_in(streams_of[7], 71), 0)
    return dict(leaf_rhs=leaf_rhs, leaf_inverse=leaf_inverse, leaf_lower=leaf_lower, sep_rhs=sep_rhs, sep_inverse=sep_inverse, sep_lower=sep_lower, slot_map=slot_map)


HIGH = lax.Precision.HIGHEST


def product_f32(matrix, vectors):
    return jnp.dot(matrix.astype(jnp.float32), vectors.astype(jnp.float32), precision=HIGH)


def leaf_node(operands):
    inverse, lower_part, front_rows = operands
    solved = product_f32(inverse, front_rows).astype(jnp.bfloat16)
    return solved, -product_f32(lower_part, solved)


def node_solve(operands):
    return product_f32(operands[0], operands[1]).astype(jnp.bfloat16)


def node_reduce(operands):
    return product_f32(operands[0], operands[1])


def reference(leaf_rhs, leaf_inverse, leaf_lower, sep_rhs, sep_inverse, sep_lower, slot_map):
    leaf_front = leaf_rhs.reshape(N_LEAF, SN0, RHS)
    leaf_inv = leaf_inverse.reshape(N_LEAF, SN0, SN0)
    leaf_low = leaf_lower.reshape(N_LEAF, UPD_DEV * N_BLK, SN0)
    leaf_solution, update = lax.map(leaf_node, (leaf_inv, leaf_low, leaf_front))
    update = update.reshape(POS, 2, PIV_DEV, RHS)
    solutions = []
    for height in range(1, LV + 1):
        at_root = height == LV
        front_slots = 1 if at_root else 3
        targets = slot_map[height - 1]
        onehot = (targets[:, :, None] == jnp.arange(2 * front_slots, dtype=jnp.int32)[None, None, :]).astype(jnp.float32)
        mixed = jnp.einsum("qst,qspr->qtpr", onehot, update, precision=HIGH)
        own_part = mixed[:, :front_slots]
        sent_part = mixed[:, front_slots:]
        partner = jnp.bitwise_xor(jnp.arange(POS, dtype=jnp.int32), N_BLK * 2 ** (height - 1))
        front_rows = own_part + sent_part[partner]
        pivots = (sep_rhs[height - 1].reshape(POS, PIV_DEV, RHS).astype(jnp.float32) + front_rows[:, 0]).astype(jnp.bfloat16)
        width_now = SEP_UNIT * 2 ** height
        offset = SEP_UNIT * (2 ** height - 2)
        node_count = (POS * PIV_DEV) // width_now
        inverse = sep_inverse[:, offset:offset + width_now].reshape(node_count, width_now, width_now)
        solved = lax.map(node_solve, (inverse, pivots.reshape(node_count, width_now, RHS)))
        solutions.append(solved.reshape(POS * PIV_DEV, RHS))
        if not at_root:
            lower_part = sep_lower[:, offset:offset + width_now].reshape(node_count, 2 * width_now, width_now)
            product = lax.map(node_reduce, (lower_part, solved))
            remaining = front_rows[:, 1:].reshape(node_count, 2 * width_now, RHS)
            update = (remaining - product).reshape(POS, 2, PIV_DEV, RHS)
    return leaf_solution.reshape(N_LEAF * SN0, RHS), jnp.stack(solutions)
```

```python
import jax
import jax.numpy as jnp
from jax import lax
from jax.sharding import PartitionSpec as P

DIRECT_LIMIT = 16


def exchange(value, leaf_mask, blk_mask):
    leaves = lax.axis_size("leaf")
    blks = lax.axis_size("blk")
    pairs = [
        (k * blks + b, (k ^ leaf_mask) * blks + (b ^ blk_mask))
        for k in range(leaves)
        for b in range(blks)
    ]
    return lax.ppermute(value, ("leaf", "blk"), pairs)


def product(matrix, vectors):
    return jnp.dot(matrix, vectors, preferred_element_type=jnp.float32)


def on_device(leaf_rhs, leaf_inverse, leaf_lower, sep_rhs, sep_inverse, sep_lower, slot_map):
    leaves = lax.axis_size("leaf")
    blks = lax.axis_size("blk")
    chips = blks // 2
    k = lax.axis_index("leaf")
    b = lax.axis_index("blk")
    z = b // 2
    core = b % 2
    half = leaf_rhs.shape[1] // 2
    levels, pivots = sep_rhs.shape[0], sep_rhs.shape[1]
    base_width = pivots * blks
    rows = leaf_rhs.shape[0]
    dtype = leaf_rhs.dtype

    def columns_of(value, which):
        return lax.dynamic_slice_in_dim(value, which * half, half, value.ndim - 1)

    def in_order(mine, other, axis=0):
        first = jnp.where(core == 0, mine, other)
        second = jnp.where(core == 0, other, mine)
        return jnp.concatenate([first, second], axis=axis)

    def put(buffer, piece, index):
        return lax.dynamic_update_slice_in_dim(buffer, piece, index * piece.shape[0], 0)

    own_half = columns_of(leaf_rhs, core)
    other_half = columns_of(leaf_rhs, 1 - core)
    rhs = put(jnp.zeros((blks * rows, half), dtype), own_half, b)
    arrived = {}
    for mask in range(1, blks):
        arrived[mask] = exchange(own_half if mask % 2 == 0 else other_half, 0, mask)
    inverse_other = exchange(leaf_inverse, 0, 1)
    lower_other = exchange(leaf_lower, 0, 1)
    sep_inverse_other = exchange(sep_inverse, 0, 1)
    sep_lower_other = exchange(sep_lower, 0, 1)
    slot_other = exchange(slot_map, 0, 1)
    sep_rhs_other = exchange(columns_of(sep_rhs, 1 - core), 0, 1)
    for mask in range(1, blks):
        rhs = put(rhs, arrived[mask], b ^ mask)

    slots = in_order(slot_map, slot_other, 1)
    seps = in_order(columns_of(sep_rhs, core), sep_rhs_other, 1)
    inv_chip = in_order(sep_inverse, sep_inverse_other)
    low_chip = in_order(sep_lower, sep_lower_other)

    top_mask = 2 ** (levels - 1)
    top_width = base_width * 2**levels
    top_offset = base_width * (2**levels - 2)
    top = sep_inverse[:, top_offset:]

    def leaf_columns(leaf_index):
        near = lax.dynamic_slice_in_dim(top, leaf_index * base_width, base_width, 1)
        far = lax.dynamic_slice_in_dim(top, (leaf_index ^ top_mask) * base_width, base_width, 1)
        return jnp.concatenate([near, far], axis=1)

    top_mine = jnp.stack(
        [leaf_columns(k)] + [exchange(leaf_columns(k ^ a), a, 0) for a in range(1, leaves)]
    )
    top_other = exchange(top_mine, 0, 1)
    top_rows = jnp.concatenate([top_mine, top_other], axis=0).reshape(-1, 2 * base_width)

    s_mine = product(leaf_inverse, rhs).astype(dtype)
    s_other = product(inverse_other, rhs).astype(dtype)
    s_all = put(put(jnp.zeros((blks * rows, half), dtype), s_mine, b), s_other, b ^ 1)
    got = [(m, exchange(s_mine, 0, m), exchange(s_other, 0, m)) for m in range(2, blks, 2)]
    for m, near, far in got:
        s_all = put(put(s_all, near, b ^ m), far, b ^ m ^ 1)
    leaf_back = exchange(s_other, 0, 1)
    leaf_solution = in_order(s_mine, leaf_back, 1)
    update = -in_order(product(leaf_lower, s_all), product(lower_other, s_all))

    def gather_z(piece):
        pieces = [piece] + [exchange(piece, 0, m) for m in range(2, blks, 2)]
        result = jnp.zeros((chips,) + piece.shape, piece.dtype)
        for m, value in enumerate(pieces):
            result = lax.dynamic_update_slice_in_dim(result, value[None], z ^ m, 0)
        return result

    def gather_node(piece, height):
        members = 2**height
        place = k % members
        if members * chips <= DIRECT_LIMIT:
            result = jnp.zeros((members * chips,) + piece.shape, piece.dtype)
            pieces = []
            for a in range(members):
                for m in range(chips):
                    value = piece if a == 0 and m == 0 else exchange(piece, a, 2 * m)
                    pieces.append(((place ^ a) * chips + (z ^ m), value))
            for where, value in pieces:
                result = lax.dynamic_update_slice_in_dim(result, value[None], where, 0)
            return result.reshape(-1, piece.shape[-1])
        joined = piece[None]
        for bit in range(height):
            theirs = exchange(joined, 2**bit, 0)
            upper = (k // 2**bit) % 2 == 1
            joined = jnp.concatenate(
                [jnp.where(upper, theirs, joined), jnp.where(upper, joined, theirs)], axis=0
            )
        return jnp.swapaxes(gather_z(joined), 0, 1).reshape(-1, piece.shape[-1])

    def mix(slot_rows, targets, count):
        result = []
        for t in count:
            hit = (targets == t)[:, :, None, None]
            result.append(jnp.sum(jnp.where(hit, slot_rows, 0), axis=1).reshape(-1, half))
        return result

    solutions = []
    for height in range(1, levels):
        mask = 2 ** (height - 1)
        offset = base_width * (2**height - 2)
        width = base_width * 2**height
        targets = slots[height - 1]
        slot_rows = update.reshape(2, 2, pivots, half)
        theirs = exchange(slot_rows.astype(dtype), mask, 0)
        their_targets = exchange(slot_map[height - 1], mask, 0)
        their_other = exchange(their_targets, 0, 1)
        their_targets = in_order(their_targets, their_other)
        own = mix(slot_rows, targets, range(3))
        sent = mix(theirs.astype(jnp.float32), their_targets, range(3, 6))
        front = [x + y for x, y in zip(own, sent)]
        pivot = (seps[height - 1].astype(jnp.float32) + front[0]).astype(dtype)
        solved = product(inv_chip[:, offset : offset + width], gather_node(pivot, height)).astype(
            dtype
        )
        solutions.append(solved)
        reduced = product(low_chip[:, offset : offset + width], gather_node(solved, height))
        rest = jnp.stack(
            [front[1].reshape(2, pivots, half), front[2].reshape(2, pivots, half)], axis=1
        )
        update = rest.reshape(-1, half) - reduced

    own, sent = mix(update.reshape(2, 2, pivots, half), slots[levels - 1], range(2))
    own = own + seps[levels - 1].astype(jnp.float32)
    parts = gather_z(jnp.stack([own, sent]).astype(dtype))
    contributions = jnp.swapaxes(parts, 0, 1).reshape(-1, half)
    partial = product(top_rows, contributions).reshape(2, leaves, pivots, half)
    rounded = partial.astype(dtype)
    near, far = partial[0, 0], None
    for a in range(1, leaves):
        near = near + exchange(rounded[0, a], a, 0).astype(jnp.float32)
    for a in range(leaves):
        value = exchange(rounded[1, a], a, 1).astype(jnp.float32)
        far = value if far is None else far + value
    top_solution = in_order(near, far, 1).astype(dtype)

    outs = []
    for solved in solutions:
        mine = lax.dynamic_slice_in_dim(solved, core * pivots, pivots, 0)
        other = lax.dynamic_slice_in_dim(solved, (1 - core) * pivots, pivots, 0)
        outs.append(in_order(mine, exchange(other, 0, 1), 1))
    return leaf_solution, jnp.stack(outs + [top_solution])


def solution(mesh):
    return jax.shard_map(
        on_device,
        mesh=mesh,
        in_specs=(
            P(("leaf", "blk"), None),
            P(("leaf", "blk"), None),
            P(("leaf", "blk"), None),
            P(None, ("leaf", "blk"), None),
            P(("leaf", "blk"), None),
            P(("leaf", "blk"), None),
            P(None, ("leaf", "blk"), None),
        ),
        out_specs=(P(("leaf", "blk"), None), P(None, ("leaf", "blk"), None)),
        check_vma=False,
    )
```

```python
import jax
import jax.numpy as jnp
from jax import lax
from jax.experimental import pallas as pl
from jax.experimental.pallas import tpu as pltpu
from jax.sharding import PartitionSpec as P


DIRECT_LIMIT = 16


def exchange(value, leaf_mask, blk_mask):
    leaves = lax.axis_size("leaf")
    blks = lax.axis_size("blk")
    pairs = [
        (k * blks + b, (k ^ leaf_mask) * blks + (b ^ blk_mask))
        for k in range(leaves)
        for b in range(blks)
    ]
    return lax.ppermute(value, ("leaf", "blk"), pairs)


def product(matrix, vectors):
    return jnp.dot(matrix, vectors, preferred_element_type=jnp.float32)


def leaf_solve(pieces, near, far):
    count = len(pieces)
    rows, half = pieces[0].shape
    dtype = pieces[0].dtype

    def body(*refs):
        piece_refs = refs[:count]
        near_ref, far_ref = refs[count : count + 2]
        all_ref, mine_ref, other_ref = refs[count + 2 : count + 5]
        rhs, near_vmem, far_vmem, sems = refs[count + 5 :]
        b = lax.axis_index("blk")
        core = b % 2
        copies = []
        for mask in range(count):
            where = pl.multiple_of((b ^ mask) * rows, 16)
            copies.append(
                pltpu.make_async_copy(
                    piece_refs[mask], rhs.at[pl.ds(where, rows)], sems.at[mask]
                )
            )
        near_copy = pltpu.make_async_copy(near_ref, near_vmem, sems.at[count])
        far_copy = pltpu.make_async_copy(far_ref, far_vmem, sems.at[count + 1])
        for copy in copies:
            copy.start()
        near_copy.start()
        far_copy.start()
        for copy in copies:
            copy.wait()
        near_copy.wait()
        mine = jnp.dot(near_vmem[...], rhs[...], preferred_element_type=jnp.float32).astype(dtype)
        mine_ref[...] = mine
        all_ref[pl.ds(pl.multiple_of(core * rows, 16), rows)] = mine
        far_copy.wait()
        other = jnp.dot(far_vmem[...], rhs[...], preferred_element_type=jnp.float32).astype(dtype)
        other_ref[...] = other
        all_ref[pl.ds(pl.multiple_of((1 - core) * rows, 16), rows)] = other

    vmem = pl.BlockSpec(memory_space=pltpu.VMEM)
    return pl.pallas_call(
        body,
        in_specs=[pl.BlockSpec(memory_space=pl.ANY)] * (count + 2),
        out_specs=[vmem] * 3,
        out_shape=[
            jax.ShapeDtypeStruct((2 * rows, half), dtype),
            jax.ShapeDtypeStruct((rows, half), dtype),
            jax.ShapeDtypeStruct((rows, half), dtype),
        ],
        scratch_shapes=[
            pltpu.VMEM((count * rows, half), dtype),
            pltpu.VMEM(near.shape, dtype),
            pltpu.VMEM(far.shape, dtype),
            pltpu.SemaphoreType.DMA((count + 2,)),
        ],
        cost_estimate=pl.CostEstimate(
            flops=4 * rows * count * rows * half, bytes_accessed=2 * near.size * 2, transcendentals=0
        ),
        name="leaf_solve",
    )(*pieces, near, far)


def on_device(leaf_rhs, leaf_inverse, leaf_lower, sep_rhs, sep_inverse, sep_lower, slot_map):
    leaves = lax.axis_size("leaf")
    blks = lax.axis_size("blk")
    chips = blks // 2
    k = lax.axis_index("leaf")
    b = lax.axis_index("blk")
    z = b // 2
    core = b % 2
    half = leaf_rhs.shape[1] // 2
    levels, pivots = sep_rhs.shape[0], sep_rhs.shape[1]
    base_width = pivots * blks
    rows = leaf_rhs.shape[0]
    dtype = leaf_rhs.dtype

    def columns_of(value, which):
        return lax.dynamic_slice_in_dim(value, which * half, half, value.ndim - 1)

    def in_order(mine, other, axis=0):
        first = jnp.where(core == 0, mine, other)
        second = jnp.where(core == 0, other, mine)
        return jnp.concatenate([first, second], axis=axis)

    def put(buffer, piece, index):
        return lax.dynamic_update_slice_in_dim(buffer, piece, index * piece.shape[0], 0)

    own_half = columns_of(leaf_rhs, core)
    other_half = columns_of(leaf_rhs, 1 - core)
    arrived = [own_half]
    for mask in range(1, blks):
        arrived.append(exchange(own_half if mask % 2 == 0 else other_half, 0, mask))
    inverse_other = exchange(leaf_inverse, 0, 1)
    lower_other = exchange(leaf_lower, 0, 1)
    slot_other = exchange(slot_map, 0, 1)
    sep_rhs_other = exchange(columns_of(sep_rhs, 1 - core), 0, 1)
    sep_lower_other = exchange(sep_lower, 0, 1)
    sep_inverse_other = exchange(sep_inverse, 0, 1)

    slots = in_order(slot_map, slot_other, 1)
    seps = in_order(columns_of(sep_rhs, core), sep_rhs_other, 1)

    s_all, s_mine, s_other = leaf_solve(arrived, leaf_inverse, inverse_other)
    got = [(m, exchange(s_all, 0, m)) for m in range(blks - 2, 0, -2)]
    s_full = put(jnp.zeros((blks * rows, half), dtype), s_all, z)
    for m, value in got:
        s_full = put(s_full, value, z ^ (m // 2))

    inv_chip = in_order(sep_inverse, sep_inverse_other)
    low_chip = in_order(sep_lower, sep_lower_other)

    top_mask = 2 ** (levels - 1)
    top_offset = base_width * (2**levels - 2)
    top = sep_inverse[:, top_offset:]

    def leaf_columns(leaf_index):
        near = lax.dynamic_slice_in_dim(top, leaf_index * base_width, base_width, 1)
        far = lax.dynamic_slice_in_dim(top, (leaf_index ^ top_mask) * base_width, base_width, 1)
        return jnp.concatenate([near, far], axis=1)

    paired = levels > 1
    blocks = [leaf_columns(k)[None]]
    for a in range(1, leaves):
        block = leaf_columns(k ^ a)[None]
        if a == 1 and paired:
            block = jnp.concatenate([sep_inverse[None, :, : 2 * base_width], block])
        blocks.append(exchange(block, a, 0))
    mine = jnp.concatenate(blocks)
    other = exchange(mine, 0, 1)
    if paired:
        their_slots = exchange(slots[0], 1, 0)
        their_sep = exchange(seps[0], 1, 0)
        inv_theirs = in_order(mine[1], other[1])
        mine = jnp.concatenate([mine[:1], mine[2:]])
        other = jnp.concatenate([other[:1], other[2:]])
    first = jnp.where(core == 0, mine, other)
    second = jnp.where(core == 0, other, mine)
    top_rows = jnp.stack([first, second], axis=1).reshape(-1, 2 * base_width)

    update = -in_order(product(leaf_lower, s_full), product(lower_other, s_full))
    leaf_back = exchange(s_other, 0, 1)
    leaf_solution = in_order(s_mine, leaf_back, 1)

    def gather_z(piece):
        pieces = [piece] + [exchange(piece, 0, m) for m in range(2, blks, 2)]
        result = jnp.zeros((chips,) + piece.shape, piece.dtype)
        for m, value in enumerate(pieces):
            result = lax.dynamic_update_slice_in_dim(result, value[None], z ^ m, 0)
        return result

    def gather_node(piece, height):
        members = 2**height
        place = k % members
        if members * chips <= DIRECT_LIMIT:
            result = jnp.zeros((members * chips,) + piece.shape, piece.dtype)
            pieces = []
            for a in range(members):
                for m in range(chips):
                    value = piece if a == 0 and m == 0 else exchange(piece, a, 2 * m)
                    pieces.append(((place ^ a) * chips + (z ^ m), value))
            for where, value in pieces:
                result = lax.dynamic_update_slice_in_dim(result, value[None], where, 0)
            return result.reshape(-1, piece.shape[-1])
        joined = piece[None]
        for bit in range(height):
            theirs = exchange(joined, 2**bit, 0)
            upper = (k // 2**bit) % 2 == 1
            joined = jnp.concatenate(
                [jnp.where(upper, theirs, joined), jnp.where(upper, joined, theirs)], axis=0
            )
        return jnp.swapaxes(gather_z(joined), 0, 1).reshape(-1, piece.shape[-1])

    def mix(slot_rows, targets, count):
        result = []
        for t in count:
            hit = (targets == t)[:, :, None, None]
            result.append(jnp.sum(jnp.where(hit, slot_rows, 0), axis=1).reshape(-1, half))
        return result

    def rest_rows(front):
        slots_of = [value.reshape(2, pivots, half) for value in front]
        return jnp.stack(slots_of, axis=1).reshape(-1, half)

    solutions = []
    for height in range(1, levels):
        mask = 2 ** (height - 1)
        offset = base_width * (2**height - 2)
        width = base_width * 2**height
        targets = slots[height - 1]
        slot_rows = update.reshape(2, 2, pivots, half)
        theirs = exchange(slot_rows.astype(dtype), mask, 0).astype(jnp.float32)
        their_targets = their_slots if height == 1 else exchange(targets, mask, 0)
        own = mix(slot_rows, targets, range(3))
        sent = mix(theirs, their_targets, range(3, 6))
        pivot = (seps[height - 1].astype(jnp.float32) + own[0] + sent[0]).astype(dtype)
        rest = rest_rows([own[1] + sent[1], own[2] + sent[2]])
        inverse_here = inv_chip[:, offset : offset + width]
        if height == 1:
            upper = k % 2 == 1

            def by_leaf(near, far):
                return jnp.stack([jnp.where(upper, far, near), jnp.where(upper, near, far)])

            (their_own,) = mix(theirs, their_targets, range(1))
            (their_sent,) = mix(slot_rows, targets, range(3, 4))
            their_pivot = (their_sep.astype(jnp.float32) + their_own + their_sent).astype(dtype)
            pivots_all = gather_z(by_leaf(pivot, their_pivot))
            pivots_all = jnp.swapaxes(pivots_all, 0, 1).reshape(-1, half)
            solved = product(inverse_here, pivots_all).astype(dtype)
            their_solved = product(inv_theirs, pivots_all).astype(dtype)
            solved_all = gather_z(by_leaf(solved, their_solved))
            solved_all = jnp.swapaxes(solved_all, 0, 1).reshape(-1, half)
        else:
            solved = product(inverse_here, gather_node(pivot, height)).astype(dtype)
            solved_all = gather_node(solved, height)
        solutions.append(solved)
        update = rest - product(low_chip[:, offset : offset + width], solved_all)

    own, sent = mix(update.reshape(2, 2, pivots, half), slots[levels - 1], range(2))
    own = own + seps[levels - 1].astype(jnp.float32)
    parts = gather_z(jnp.stack([own, sent]).astype(dtype))
    contributions = jnp.swapaxes(parts, 0, 1).reshape(-1, half)
    partial = product(top_rows, contributions).reshape(leaves, 2 * pivots, half)
    rounded = partial.astype(dtype)
    total = partial[0]
    for a in range(1, leaves):
        total = total + exchange(rounded[a], a, 0).astype(jnp.float32)
    solutions.append(total.astype(dtype))

    outs = []
    for solved in solutions:
        mine = lax.dynamic_slice_in_dim(solved, core * pivots, pivots, 0)
        other = lax.dynamic_slice_in_dim(solved, (1 - core) * pivots, pivots, 0)
        outs.append(in_order(mine, exchange(other, 0, 1), 1))
    return leaf_solution, jnp.stack(outs)


def solution(mesh):
    return jax.shard_map(
        on_device,
        mesh=mesh,
        in_specs=(
            P(("leaf", "blk"), None),
            P(("leaf", "blk"), None),
            P(("leaf", "blk"), None),
            P(None, ("leaf", "blk"), None),
            P(("leaf", "blk"), None),
            P(("leaf", "blk"), None),
            P(None, ("leaf", "blk"), None),
        ),
        out_specs=(P(("leaf", "blk"), None), P(None, ("leaf", "blk"), None)),
        check_vma=False,
    )
```

```python
import jax
import jax.numpy as jnp
from jax import lax
from jax.experimental import pallas as pl
from jax.experimental.pallas import tpu as pltpu
from jax.sharding import PartitionSpec as P


DIRECT_LIMIT = 16


def exchange(value, leaf_mask, blk_mask):
    leaves = lax.axis_size("leaf")
    blks = lax.axis_size("blk")
    pairs = [
        (k * blks + b, (k ^ leaf_mask) * blks + (b ^ blk_mask))
        for k in range(leaves)
        for b in range(blks)
    ]
    return lax.ppermute(value, ("leaf", "blk"), pairs)


def product(matrix, vectors):
    return jnp.dot(matrix, vectors, preferred_element_type=jnp.float32)


def leaf_solve(pieces, near, far):
    count = len(pieces)

    def keep_in(space, value):
        return pltpu.with_memory_space_constraint(value, space)

    rows, half = pieces[0].shape
    dtype = pieces[0].dtype

    def body(*refs):
        piece_refs = refs[:count]
        near_ref, far_ref = refs[count : count + 2]
        all_ref, mine_ref, other_ref = refs[count + 2 : count + 5]
        rhs, near_vmem, far_vmem, sems = refs[count + 5 :]
        b = lax.axis_index("blk")
        core = b % 2
        copies = [
            pltpu.make_async_copy(source, target, sems.at[i])
            for i, (source, target) in enumerate(((near_ref, near_vmem), (far_ref, far_vmem)))
        ]
        for copy in copies:
            copy.start()
        for mask in range(count):
            where = pl.multiple_of((b ^ mask) * rows, 16)
            rhs[pl.ds(where, rows)] = piece_refs[mask][...]
        copies[0].wait()
        mine = jnp.dot(near_vmem[...], rhs[...], preferred_element_type=jnp.float32).astype(dtype)
        mine_ref[...] = mine
        all_ref[pl.ds(pl.multiple_of(core * rows, 16), rows)] = mine
        copies[1].wait()
        other = jnp.dot(far_vmem[...], rhs[...], preferred_element_type=jnp.float32).astype(dtype)
        other_ref[...] = other
        all_ref[pl.ds(pl.multiple_of((1 - core) * rows, 16), rows)] = other

    vmem = pl.BlockSpec(memory_space=pltpu.VMEM)
    return pl.pallas_call(
        body,
        in_specs=[vmem] * count + [pl.BlockSpec(memory_space=pltpu.HBM)] * 2,
        out_specs=[vmem] * 3,
        out_shape=[
            pltpu.VMEM((2 * rows, half), dtype),
            pltpu.VMEM((rows, half), dtype),
            pltpu.VMEM((rows, half), dtype),
        ],
        scratch_shapes=[
            pltpu.VMEM((count * rows, half), dtype),
            pltpu.VMEM(near.shape, dtype),
            pltpu.VMEM(far.shape, dtype),
            pltpu.SemaphoreType.DMA((2,)),
        ],
        cost_estimate=pl.CostEstimate(
            flops=4 * rows * count * rows * half, bytes_accessed=2 * near.size * 2, transcendentals=0
        ),
        name="leaf_solve",
    )(*[keep_in(pltpu.VMEM, value) for value in pieces], near, keep_in(pltpu.HBM, far))


def on_device(leaf_rhs, leaf_inverse, leaf_lower, sep_rhs, sep_inverse, sep_lower, slot_map):
    leaves = lax.axis_size("leaf")
    blks = lax.axis_size("blk")
    chips = blks // 2
    k = lax.axis_index("leaf")
    b = lax.axis_index("blk")
    z = b // 2
    core = b % 2
    half = leaf_rhs.shape[1] // 2
    levels, pivots = sep_rhs.shape[0], sep_rhs.shape[1]
    base_width = pivots * blks
    rows = leaf_rhs.shape[0]
    dtype = leaf_rhs.dtype

    def columns_of(value, which):
        return lax.dynamic_slice_in_dim(value, which * half, half, value.ndim - 1)

    def in_order(mine, other, axis=0):
        first = jnp.where(core == 0, mine, other)
        second = jnp.where(core == 0, other, mine)
        return jnp.concatenate([first, second], axis=axis)

    def put(buffer, piece, index):
        return lax.dynamic_update_slice_in_dim(buffer, piece, index * piece.shape[0], 0)

    own_half = columns_of(leaf_rhs, core)
    other_half = columns_of(leaf_rhs, 1 - core)
    arrived = [own_half]
    for mask in range(1, blks):
        arrived.append(exchange(own_half if mask % 2 == 0 else other_half, 0, mask))
    inverse_other = exchange(leaf_inverse, 0, 1)
    slot_other = exchange(slot_map, 0, 1)
    sep_rhs_other = exchange(sep_rhs, 0, 1)
    lower_other = exchange(leaf_lower, 0, 1)
    sep_lower_other = exchange(sep_lower, 0, 1)
    inverse_rows = [sep_inverse] + [exchange(sep_inverse, a, 0) for a in range(1, leaves)]

    s_all, s_mine, s_other = leaf_solve(arrived, leaf_inverse, inverse_other)
    got = [(m, exchange(s_all, 0, m)) for m in range(blks - 2, 0, -2)]
    s_full = put(jnp.zeros((blks * rows, half), dtype), s_all, z)
    for m, value in got:
        s_full = put(s_full, value, z ^ (m // 2))

    inverse_others = [exchange(value, 0, 1) for value in inverse_rows]
    slots = in_order(slot_map, slot_other, 1)
    seps = in_order(columns_of(sep_rhs, core), columns_of(sep_rhs_other, core), 1)
    paired = levels > 1
    if paired:
        their_slots = exchange(slots[0], 1, 0)
        their_sep = exchange(seps[0], 1, 0)

    top_mask = 2 ** (levels - 1)
    top_offset = base_width * (2**levels - 2)
    low_chip = in_order(sep_lower, sep_lower_other)
    inv_chip = in_order(sep_inverse[:, :top_offset], inverse_others[0][:, :top_offset])
    if paired:
        inv_theirs = in_order(
            inverse_rows[1][:, : 2 * base_width], inverse_others[1][:, : 2 * base_width]
        )

    def leaf_columns(value):
        near = lax.dynamic_slice_in_dim(value, top_offset + k * base_width, base_width, 1)
        far = lax.dynamic_slice_in_dim(
            value, top_offset + (k ^ top_mask) * base_width, base_width, 1
        )
        return jnp.concatenate([near, far], axis=1)

    top_rows = jnp.concatenate(
        [
            in_order(leaf_columns(mine), leaf_columns(other))
            for mine, other in zip(inverse_rows, inverse_others)
        ]
    )

    update = -in_order(product(leaf_lower, s_full), product(lower_other, s_full))
    leaf_back = exchange(s_other, 0, 1)
    leaf_solution = in_order(s_mine, leaf_back, 1)

    def gather_z(piece):
        pieces = [piece] + [exchange(piece, 0, m) for m in range(blks - 2, 0, -2)]
        result = jnp.zeros((chips,) + piece.shape, piece.dtype)
        for m, value in zip([0] + list(range(chips - 1, 0, -1)), pieces):
            result = lax.dynamic_update_slice_in_dim(result, value[None], z ^ m, 0)
        return result

    def gather_node(piece, height):
        members = 2**height
        place = k % members
        if members * chips <= DIRECT_LIMIT:
            result = jnp.zeros((members * chips,) + piece.shape, piece.dtype)
            pieces = []
            for a in range(members):
                for m in range(chips):
                    value = piece if a == 0 and m == 0 else exchange(piece, a, 2 * m)
                    pieces.append(((place ^ a) * chips + (z ^ m), value))
            for where, value in pieces:
                result = lax.dynamic_update_slice_in_dim(result, value[None], where, 0)
            return result.reshape(-1, piece.shape[-1])
        joined = piece[None]
        for bit in range(height):
            theirs = exchange(joined, 2**bit, 0)
            upper = (k // 2**bit) % 2 == 1
            joined = jnp.concatenate(
                [jnp.where(upper, theirs, joined), jnp.where(upper, joined, theirs)], axis=0
            )
        return jnp.swapaxes(gather_z(joined), 0, 1).reshape(-1, piece.shape[-1])

    def mix(slot_rows, targets, count):
        result = []
        for t in count:
            hit = (targets == t)[:, :, None, None]
            result.append(jnp.sum(jnp.where(hit, slot_rows, 0), axis=1).reshape(-1, half))
        return result

    def rest_rows(front):
        slots_of = [value.reshape(2, pivots, half) for value in front]
        return jnp.stack(slots_of, axis=1).reshape(-1, half)

    solutions = []
    for height in range(1, levels):
        mask = 2 ** (height - 1)
        offset = base_width * (2**height - 2)
        width = base_width * 2**height
        targets = slots[height - 1]
        slot_rows = update.reshape(2, 2, pivots, half)
        theirs = exchange(slot_rows.astype(dtype), mask, 0).astype(jnp.float32)
        their_targets = their_slots if height == 1 else exchange(targets, mask, 0)
        own = mix(slot_rows, targets, range(3))
        sent = mix(theirs, their_targets, range(3, 6))
        pivot = (seps[height - 1].astype(jnp.float32) + own[0] + sent[0]).astype(dtype)
        rest = rest_rows([own[1] + sent[1], own[2] + sent[2]])
        inverse_here = inv_chip[:, offset : offset + width]
        if height == 1:
            upper = k % 2 == 1

            def by_leaf(near, far):
                return jnp.stack([jnp.where(upper, far, near), jnp.where(upper, near, far)])

            (their_own,) = mix(theirs, their_targets, range(1))
            (their_sent,) = mix(slot_rows, targets, range(3, 4))
            their_pivot = (their_sep.astype(jnp.float32) + their_own + their_sent).astype(dtype)
            pivots_all = gather_z(by_leaf(pivot, their_pivot))
            pivots_all = jnp.swapaxes(pivots_all, 0, 1).reshape(-1, half)
            solved = product(inverse_here, pivots_all).astype(dtype)
            their_solved = product(inv_theirs, pivots_all).astype(dtype)
            solved_all = gather_z(by_leaf(solved, their_solved))
            solved_all = jnp.swapaxes(solved_all, 0, 1).reshape(-1, half)
        else:
            solved = product(inverse_here, gather_node(pivot, height)).astype(dtype)
            solved_all = gather_node(solved, height)
        solutions.append(solved)
        update = rest - product(low_chip[:, offset : offset + width], solved_all)

    own, sent = mix(update.reshape(2, 2, pivots, half), slots[levels - 1], range(2))
    own = own + seps[levels - 1].astype(jnp.float32)
    parts = gather_z(jnp.stack([own, sent]).astype(dtype))
    contributions = jnp.swapaxes(parts, 0, 1).reshape(-1, half)
    partial = product(top_rows, contributions).reshape(leaves, 2 * pivots, half)
    rounded = partial.astype(dtype)
    total = partial[0]
    for a in range(1, leaves):
        total = total + exchange(rounded[a], a, 0).astype(jnp.float32)
    solutions.append(total.astype(dtype))

    outs = []
    for solved in solutions:
        mine = lax.dynamic_slice_in_dim(solved, core * pivots, pivots, 0)
        other = lax.dynamic_slice_in_dim(solved, (1 - core) * pivots, pivots, 0)
        outs.append(in_order(mine, exchange(other, 0, 1), 1))
    return leaf_solution, jnp.stack(outs)


def solution(mesh):
    return jax.shard_map(
        on_device,
        mesh=mesh,
        in_specs=(
            P(("leaf", "blk"), None),
            P(("leaf", "blk"), None),
            P(("leaf", "blk"), None),
            P(None, ("leaf", "blk"), None),
            P(("leaf", "blk"), None),
            P(("leaf", "blk"), None),
            P(None, ("leaf", "blk"), None),
        ),
        out_specs=(P(("leaf", "blk"), None), P(None, ("leaf", "blk"), None)),
        check_vma=False,
    )
```

```python
import jax
import jax.numpy as jnp
from jax import lax
from jax.experimental import pallas as pl
from jax.experimental.pallas import tpu as pltpu
from jax.sharding import PartitionSpec as P


DIRECT_LIMIT = 16


def exchange(value, leaf_mask, blk_mask):
    leaves = lax.axis_size("leaf")
    blks = lax.axis_size("blk")
    pairs = [
        (k * blks + b, (k ^ leaf_mask) * blks + (b ^ blk_mask))
        for k in range(leaves)
        for b in range(blks)
    ]
    return lax.ppermute(value, ("leaf", "blk"), pairs)


def product(matrix, vectors):
    return jnp.dot(matrix, vectors, preferred_element_type=jnp.float32)


def on_chip(value):
    return pltpu.with_memory_space_constraint(value, pltpu.VMEM)


def vmem_specs(count):
    return [pl.BlockSpec(memory_space=pltpu.VMEM)] * count


def leaf_partial(pieces, near, far):
    masks = sorted(pieces)
    count = len(masks)
    rows, half = pieces[0].shape
    total = near.shape[1]
    dtype = near.dtype

    def body(*refs):
        piece_refs = refs[:count]
        near_ref, far_ref, sum_ref, rest_ref, rhs, near_vmem, far_vmem, sems = refs[count:]
        b = lax.axis_index("blk")
        copies = [
            pltpu.make_async_copy(source, target, sems.at[i])
            for i, (source, target) in enumerate(((near_ref, near_vmem), (far_ref, far_vmem)))
        ]
        for copy in copies:
            copy.start()
        missing = pl.multiple_of((b // 2 ^ 1) * 2 * rows, 128)
        rhs[pl.ds(missing, 2 * rows)] = jnp.zeros((2 * rows, half), dtype)
        for mask, piece_ref in zip(masks, piece_refs):
            where = pl.multiple_of((b ^ mask) * rows, 16)
            rhs[pl.ds(where, rows)] = piece_ref[...]
        for i, matrix in enumerate((near_vmem, far_vmem)):
            copies[i].wait()
            sum_ref[i] = jnp.dot(matrix[...], rhs[...], preferred_element_type=jnp.float32)
            rest_ref[i] = matrix[:, pl.ds(missing, 2 * rows)]

    return pl.pallas_call(
        body,
        in_specs=vmem_specs(count) + [pl.BlockSpec(memory_space=pltpu.HBM)] * 2,
        out_specs=vmem_specs(2),
        out_shape=[
            pltpu.VMEM((2, rows, half), jnp.float32),
            pltpu.VMEM((2, rows, 2 * rows), dtype),
        ],
        scratch_shapes=[
            pltpu.VMEM((total, half), dtype),
            pltpu.VMEM(near.shape, dtype),
            pltpu.VMEM(far.shape, dtype),
            pltpu.SemaphoreType.DMA((2,)),
        ],
        cost_estimate=pl.CostEstimate(
            flops=4 * rows * total * half, bytes_accessed=4 * near.size, transcendentals=0
        ),
        name="leaf_partial",
    )(
        *[on_chip(pieces[mask]) for mask in masks],
        near,
        pltpu.with_memory_space_constraint(far, pltpu.HBM),
    )


def leaf_finish(same, cross, sums, rest):
    rows, half = same.shape
    dtype = same.dtype

    def body(same_ref, cross_ref, sum_ref, rest_ref, all_ref, mine_ref, other_ref, rhs):
        core = lax.axis_index("blk") % 2
        low = pl.multiple_of(core * rows, 16)
        high = pl.multiple_of((1 - core) * rows, 16)
        rhs[pl.ds(low, rows)] = same_ref[...]
        rhs[pl.ds(high, rows)] = cross_ref[...]
        for i, (where, out_ref) in enumerate(((low, mine_ref), (high, other_ref))):
            value = jnp.dot(rest_ref[i], rhs[...], preferred_element_type=jnp.float32)
            value = (value + sum_ref[i]).astype(dtype)
            out_ref[...] = value
            all_ref[pl.ds(where, rows)] = value

    return pl.pallas_call(
        body,
        in_specs=vmem_specs(4),
        out_specs=vmem_specs(3),
        out_shape=[
            pltpu.VMEM((2 * rows, half), dtype),
            pltpu.VMEM((rows, half), dtype),
            pltpu.VMEM((rows, half), dtype),
        ],
        scratch_shapes=[pltpu.VMEM((2 * rows, half), dtype)],
        cost_estimate=pl.CostEstimate(
            flops=8 * rows * rows * half, bytes_accessed=0, transcendentals=0
        ),
        name="leaf_finish",
    )(on_chip(same), on_chip(cross), on_chip(sums), on_chip(rest))


def on_device(leaf_rhs, leaf_inverse, leaf_lower, sep_rhs, sep_inverse, sep_lower, slot_map):
    leaves = lax.axis_size("leaf")
    blks = lax.axis_size("blk")
    chips = blks // 2
    k = lax.axis_index("leaf")
    b = lax.axis_index("blk")
    z = b // 2
    core = b % 2
    half = leaf_rhs.shape[1] // 2
    levels, pivots = sep_rhs.shape[0], sep_rhs.shape[1]
    base_width = pivots * blks
    rows = leaf_rhs.shape[0]
    dtype = leaf_rhs.dtype

    def columns_of(value, which):
        return lax.dynamic_slice_in_dim(value, which * half, half, value.ndim - 1)

    def in_order(mine, other, axis=0):
        first = jnp.where(core == 0, mine, other)
        second = jnp.where(core == 0, other, mine)
        return jnp.concatenate([first, second], axis=axis)

    def put(buffer, piece, index):
        return lax.dynamic_update_slice_in_dim(buffer, piece, index * piece.shape[0], 0)

    top_mask = 2 ** (levels - 1)
    top_offset = base_width * (2**levels - 2)
    send_whole = leaves <= DIRECT_LIMIT // 2

    def leaf_columns(value, leaf):
        near = lax.dynamic_slice_in_dim(value, top_offset + leaf * base_width, base_width, 1)
        far = lax.dynamic_slice_in_dim(
            value, top_offset + (leaf ^ top_mask) * base_width, base_width, 1
        )
        return jnp.concatenate([near, far], axis=1)

    own_half = columns_of(leaf_rhs, core)
    other_half = columns_of(leaf_rhs, 1 - core)
    arrived = {0: own_half}
    for mask in list(range(blks - 1, 3, -1)) + [1, 3, 2]:
        arrived[mask] = exchange(own_half if mask % 2 == 0 else other_half, 0, mask)
    inverse_other = exchange(leaf_inverse, 0, 1)
    slot_other = exchange(slot_map, 0, 1)
    sep_rhs_other = exchange(sep_rhs, 0, 1)
    lower_other = exchange(leaf_lower, 0, 1)
    sep_lower_other = exchange(sep_lower, 0, 1)
    inverse_rows = [sep_inverse]
    for a in range(1, leaves):
        value = sep_inverse
        if not send_whole:
            value = jnp.concatenate([value[:, : 2 * base_width], leaf_columns(value, k ^ a)], 1)
        inverse_rows.append(exchange(value, a, 0))

    same, cross = arrived.pop(2), arrived.pop(3)
    sums, beside = leaf_partial(arrived, leaf_inverse, inverse_other)
    s_all, s_mine, s_other = leaf_finish(same, cross, sums, beside)
    got = [(m, exchange(s_all, 0, m)) for m in range(blks - 2, 0, -2)]
    s_full = put(jnp.zeros((blks * rows, half), dtype), s_all, z)
    for m, value in got:
        s_full = put(s_full, value, z ^ (m // 2))

    inverse_others = [exchange(value, 0, 1) for value in inverse_rows]
    slots = in_order(slot_map, slot_other, 1)
    seps = in_order(columns_of(sep_rhs, core), columns_of(sep_rhs_other, core), 1)
    paired = levels > 1
    if paired:
        their_slots = exchange(slots[0], 1, 0)
        their_sep = exchange(seps[0], 1, 0)

    low_chip = in_order(sep_lower, sep_lower_other)
    inv_chip = in_order(sep_inverse[:, :top_offset], inverse_others[0][:, :top_offset])
    if paired:
        inv_theirs = in_order(
            inverse_rows[1][:, : 2 * base_width], inverse_others[1][:, : 2 * base_width]
        )

    def top_columns(a, value):
        return leaf_columns(value, k) if a == 0 or send_whole else value[:, 2 * base_width :]

    top_rows = jnp.concatenate(
        [
            in_order(top_columns(a, mine), top_columns(a, other))
            for a, (mine, other) in enumerate(zip(inverse_rows, inverse_others))
        ]
    )

    update = -in_order(product(leaf_lower, s_full), product(lower_other, s_full))
    leaf_back = exchange(s_other, 0, 1)
    leaf_solution = in_order(s_mine, leaf_back, 1)

    def gather_z(piece):
        pieces = [piece] + [exchange(piece, 0, m) for m in range(blks - 2, 0, -2)]
        result = jnp.zeros((chips,) + piece.shape, piece.dtype)
        for m, value in zip([0] + list(range(chips - 1, 0, -1)), pieces):
            result = lax.dynamic_update_slice_in_dim(result, value[None], z ^ m, 0)
        return result

    def gather_node(piece, height):
        members = 2**height
        place = k % members
        if members * chips <= DIRECT_LIMIT:
            result = jnp.zeros((members * chips,) + piece.shape, piece.dtype)
            pieces = []
            for a in range(members):
                for m in range(chips):
                    value = piece if a == 0 and m == 0 else exchange(piece, a, 2 * m)
                    pieces.append(((place ^ a) * chips + (z ^ m), value))
            for where, value in pieces:
                result = lax.dynamic_update_slice_in_dim(result, value[None], where, 0)
            return result.reshape(-1, piece.shape[-1])
        joined = piece[None]
        for bit in range(height):
            theirs = exchange(joined, 2**bit, 0)
            upper = (k // 2**bit) % 2 == 1
            joined = jnp.concatenate(
                [jnp.where(upper, theirs, joined), jnp.where(upper, joined, theirs)], axis=0
            )
        return jnp.swapaxes(gather_z(joined), 0, 1).reshape(-1, piece.shape[-1])

    def mix(slot_rows, targets, count):
        result = []
        for t in count:
            hit = (targets == t)[:, :, None, None]
            result.append(jnp.sum(jnp.where(hit, slot_rows, 0), axis=1).reshape(-1, half))
        return result

    def rest_rows(front):
        slots_of = [value.reshape(2, pivots, half) for value in front]
        return jnp.stack(slots_of, axis=1).reshape(-1, half)

    solutions = []
    for height in range(1, levels):
        mask = 2 ** (height - 1)
        offset = base_width * (2**height - 2)
        width = base_width * 2**height
        targets = slots[height - 1]
        slot_rows = update.reshape(2, 2, pivots, half)
        theirs = exchange(slot_rows.astype(dtype), mask, 0).astype(jnp.float32)
        their_targets = their_slots if height == 1 else exchange(targets, mask, 0)
        own = mix(slot_rows, targets, range(3))
        sent = mix(theirs, their_targets, range(3, 6))
        pivot = (seps[height - 1].astype(jnp.float32) + own[0] + sent[0]).astype(dtype)
        rest = rest_rows([own[1] + sent[1], own[2] + sent[2]])
        inverse_here = inv_chip[:, offset : offset + width]
        if height == 1:
            upper = k % 2 == 1

            def by_leaf(near, far):
                return jnp.stack([jnp.where(upper, far, near), jnp.where(upper, near, far)])

            (their_own,) = mix(theirs, their_targets, range(1))
            (their_sent,) = mix(slot_rows, targets, range(3, 4))
            their_pivot = (their_sep.astype(jnp.float32) + their_own + their_sent).astype(dtype)
            pivots_all = gather_z(by_leaf(pivot, their_pivot))
            pivots_all = jnp.swapaxes(pivots_all, 0, 1).reshape(-1, half)
            solved = product(inverse_here, pivots_all).astype(dtype)
            their_solved = product(inv_theirs, pivots_all).astype(dtype)
            solved_all = gather_z(by_leaf(solved, their_solved))
            solved_all = jnp.swapaxes(solved_all, 0, 1).reshape(-1, half)
        else:
            solved = product(inverse_here, gather_node(pivot, height)).astype(dtype)
            solved_all = gather_node(solved, height)
        solutions.append(solved)
        update = rest - product(low_chip[:, offset : offset + width], solved_all)

    own, sent = mix(update.reshape(2, 2, pivots, half), slots[levels - 1], range(2))
    own = own + seps[levels - 1].astype(jnp.float32)
    parts = gather_z(jnp.stack([own, sent]).astype(dtype))
    contributions = jnp.swapaxes(parts, 0, 1).reshape(-1, half)
    partial = product(top_rows, contributions).reshape(leaves, 2 * pivots, half)
    rounded = partial.astype(dtype)
    total = partial[0]
    for a in range(1, leaves):
        total = total + exchange(rounded[a], a, 0).astype(jnp.float32)
    solutions.append(total.astype(dtype))

    outs = []
    for solved in solutions:
        mine = lax.dynamic_slice_in_dim(solved, core * pivots, pivots, 0)
        other = lax.dynamic_slice_in_dim(solved, (1 - core) * pivots, pivots, 0)
        outs.append(in_order(mine, exchange(other, 0, 1), 1))
    return leaf_solution, jnp.stack(outs)


def solution(mesh):
    return jax.shard_map(
        on_device,
        mesh=mesh,
        in_specs=(
            P(("leaf", "blk"), None),
            P(("leaf", "blk"), None),
            P(("leaf", "blk"), None),
            P(None, ("leaf", "blk"), None),
            P(("leaf", "blk"), None),
            P(("leaf", "blk"), None),
            P(None, ("leaf", "blk"), None),
        ),
        out_specs=(P(("leaf", "blk"), None), P(None, ("leaf", "blk"), None)),
        check_vma=False,
    )
```

```python
import jax
import jax.numpy as jnp
from jax import lax
from jax.experimental import pallas as pl
from jax.experimental.pallas import tpu as pltpu
from jax.sharding import PartitionSpec as P


DIRECT_LIMIT = 16


def exchange(value, leaf_mask, blk_mask):
    leaves = lax.axis_size("leaf")
    blks = lax.axis_size("blk")
    pairs = [
        (k * blks + b, (k ^ leaf_mask) * blks + (b ^ blk_mask))
        for k in range(leaves)
        for b in range(blks)
    ]
    return lax.ppermute(value, ("leaf", "blk"), pairs)


def product(matrix, vectors):
    return jnp.dot(matrix, vectors, preferred_element_type=jnp.float32)


def on_chip(value):
    return pltpu.with_memory_space_constraint(value, pltpu.VMEM)


def vmem_specs(count):
    return [pl.BlockSpec(memory_space=pltpu.VMEM)] * count


def leaf_partial(pieces, near, far):
    masks = sorted(pieces)
    count = len(masks)
    rows, half = pieces[0].shape
    total = near.shape[1]
    block = 4 * rows
    flip = total // block - 1
    dtype = near.dtype

    def body(*refs):
        piece_refs = refs[:count]
        near_ref, far_ref, sum_ref, rest_ref, rhs, near_vmem, far_vmem, sems = refs[count:]
        b = lax.axis_index("blk")
        copies = [
            pltpu.make_async_copy(source, target, sems.at[i])
            for i, (source, target) in enumerate(((near_ref, near_vmem), (far_ref, far_vmem)))
        ]
        for copy in copies:
            copy.start()
        missing = pl.multiple_of((b // 4 ^ flip) * block, 128)
        rhs[pl.ds(missing, block)] = jnp.zeros((block, half), dtype)
        for mask, piece_ref in zip(masks, piece_refs):
            where = pl.multiple_of((b ^ mask) * rows, 16)
            rhs[pl.ds(where, rows)] = piece_ref[...]
        for i, matrix in enumerate((near_vmem, far_vmem)):
            copies[i].wait()
            sum_ref[i] = jnp.dot(matrix[...], rhs[...], preferred_element_type=jnp.float32)
        rest_ref[...] = near_vmem[:, pl.ds(missing, block)]

    return pl.pallas_call(
        body,
        in_specs=vmem_specs(count) + [pl.BlockSpec(memory_space=pltpu.HBM)] * 2,
        out_specs=vmem_specs(2),
        out_shape=[
            pltpu.VMEM((2, rows, half), jnp.float32),
            pltpu.VMEM((rows, block), dtype),
        ],
        scratch_shapes=[
            pltpu.VMEM((total, half), dtype),
            pltpu.VMEM(near.shape, dtype),
            pltpu.VMEM(far.shape, dtype),
            pltpu.SemaphoreType.DMA((2,)),
        ],
        cost_estimate=pl.CostEstimate(
            flops=4 * rows * total * half, bytes_accessed=4 * near.size, transcendentals=0
        ),
        name="leaf_partial",
    )(
        *[on_chip(pieces[mask]) for mask in masks],
        near,
        pltpu.with_memory_space_constraint(far, pltpu.HBM),
    )


def leaf_finish(pieces, sums, rest, far):
    count = len(pieces)
    rows, half = pieces[0].shape
    dtype = pieces[0].dtype
    flip = far.shape[1] // (count * rows) - 1

    def body(*refs):
        piece_refs = refs[:count]
        sum_ref, rest_ref, far_ref, all_ref, mine_ref, other_ref, rhs, far_vmem, sem = refs[count:]
        b = lax.axis_index("blk")
        where = pl.multiple_of((b // count ^ flip) * count * rows, 128)
        copy = pltpu.make_async_copy(far_ref.at[:, pl.ds(where, count * rows)], far_vmem, sem)
        copy.start()
        for mask, piece_ref in enumerate(piece_refs):
            where = pl.multiple_of((b % count ^ mask) * rows, 16)
            rhs[pl.ds(where, rows)] = piece_ref[...]
        for i, (matrix, out_ref) in enumerate(((rest_ref, mine_ref), (far_vmem, other_ref))):
            if i == 1:
                copy.wait()
            value = jnp.dot(matrix[...], rhs[...], preferred_element_type=jnp.float32)
            value = (value + sum_ref[i]).astype(dtype)
            out_ref[...] = value
            all_ref[pl.ds(pl.multiple_of((b % 2 ^ i) * rows, 16), rows)] = value

    return pl.pallas_call(
        body,
        in_specs=vmem_specs(count + 2) + [pl.BlockSpec(memory_space=pltpu.HBM)],
        out_specs=vmem_specs(3),
        out_shape=[
            pltpu.VMEM((2 * rows, half), dtype),
            pltpu.VMEM((rows, half), dtype),
            pltpu.VMEM((rows, half), dtype),
        ],
        scratch_shapes=[
            pltpu.VMEM((count * rows, half), dtype),
            pltpu.VMEM((rows, count * rows), dtype),
            pltpu.SemaphoreType.DMA,
        ],
        cost_estimate=pl.CostEstimate(
            flops=4 * rows * count * rows * half, bytes_accessed=0, transcendentals=0
        ),
        name="leaf_finish",
    )(
        *[on_chip(value) for value in pieces],
        on_chip(sums),
        on_chip(rest),
        pltpu.with_memory_space_constraint(far, pltpu.HBM),
    )


def column_halves(value):
    rows, half = value.shape[0], value.shape[1] // 2

    def body(value_ref, own_ref, other_ref, sems):
        core = lax.axis_index("blk") % 2
        copies = []
        for i, out_ref in enumerate((own_ref, other_ref)):
            where = pl.multiple_of((core ^ i) * half, 128)
            copies.append(
                pltpu.make_async_copy(value_ref.at[:, pl.ds(where, half)], out_ref, sems.at[i])
            )
        for copy in copies:
            copy.start()
        for copy in copies:
            copy.wait()

    return pl.pallas_call(
        body,
        in_specs=[pl.BlockSpec(memory_space=pltpu.HBM)],
        out_specs=vmem_specs(2),
        out_shape=[pltpu.VMEM((rows, half), value.dtype)] * 2,
        scratch_shapes=[pltpu.SemaphoreType.DMA((2,))],
        name="column_halves",
    )(value)


def on_device(leaf_rhs, leaf_inverse, leaf_lower, sep_rhs, sep_inverse, sep_lower, slot_map):
    leaves = lax.axis_size("leaf")
    blks = lax.axis_size("blk")
    chips = blks // 2
    k = lax.axis_index("leaf")
    b = lax.axis_index("blk")
    z = b // 2
    core = b % 2
    half = leaf_rhs.shape[1] // 2
    levels, pivots = sep_rhs.shape[0], sep_rhs.shape[1]
    base_width = pivots * blks
    rows = leaf_rhs.shape[0]
    dtype = leaf_rhs.dtype

    def columns_of(value, which):
        return lax.dynamic_slice_in_dim(value, which * half, half, value.ndim - 1)

    def in_order(mine, other, axis=0):
        first = jnp.where(core == 0, mine, other)
        second = jnp.where(core == 0, other, mine)
        return jnp.concatenate([first, second], axis=axis)

    def put(buffer, piece, index):
        return lax.dynamic_update_slice_in_dim(buffer, piece, index * piece.shape[0], 0)

    top_mask = 2 ** (levels - 1)
    top_offset = base_width * (2**levels - 2)
    send_whole = leaves <= DIRECT_LIMIT // 2

    def leaf_columns(value, leaf):
        near = lax.dynamic_slice_in_dim(value, top_offset + leaf * base_width, base_width, 1)
        far = lax.dynamic_slice_in_dim(
            value, top_offset + (leaf ^ top_mask) * base_width, base_width, 1
        )
        return jnp.concatenate([near, far], axis=1)

    inverse_other = exchange(leaf_inverse, 0, 1)
    own_half, other_half = column_halves(leaf_rhs)
    arrived = {0: own_half}
    far = list(range(blks - 4, blks))
    for mask in far[::-1] + [m for m in range(blks - 5, 1, -1)] + [1]:
        arrived[mask] = exchange(own_half if mask % 2 == 0 else other_half, 0, mask)
    inverse_rows = [sep_inverse]
    for a in range(1, leaves):
        value = sep_inverse
        if not send_whole:
            value = jnp.concatenate([value[:, : 2 * base_width], leaf_columns(value, k ^ a)], 1)
        inverse_rows.append(exchange(value, a, 0))

    last = [arrived.pop(mask) for mask in far]
    sums, beside = leaf_partial(arrived, leaf_inverse, inverse_other)
    s_all, s_mine, s_other = leaf_finish(last, sums, beside, inverse_other)
    got = [(m, exchange(s_all, 0, m)) for m in range(blks - 2, 0, -2)]
    slot_other = exchange(slot_map, 0, 1)
    sep_rhs_other = exchange(sep_rhs, 0, 1)
    lower_other = exchange(leaf_lower, 0, 1)
    sep_lower_other = exchange(sep_lower, 0, 1)
    s_full = put(jnp.zeros((blks * rows, half), dtype), s_all, z)
    for m, value in got:
        s_full = put(s_full, value, z ^ (m // 2))

    inverse_others = [exchange(value, 0, 1) for value in inverse_rows]
    slots = in_order(slot_map, slot_other, 1)
    seps = in_order(columns_of(sep_rhs, core), columns_of(sep_rhs_other, core), 1)
    paired = levels > 1
    if paired:
        their_slots = exchange(slots[0], 1, 0)
        their_sep = exchange(seps[0], 1, 0)

    low_chip = in_order(sep_lower, sep_lower_other)
    inv_chip = in_order(sep_inverse[:, :top_offset], inverse_others[0][:, :top_offset])
    if paired:
        inv_theirs = in_order(
            inverse_rows[1][:, : 2 * base_width], inverse_others[1][:, : 2 * base_width]
        )

    def top_columns(a, value):
        return leaf_columns(value, k) if a == 0 or send_whole else value[:, 2 * base_width :]

    top_rows = jnp.concatenate(
        [
            in_order(top_columns(a, mine), top_columns(a, other))
            for a, (mine, other) in enumerate(zip(inverse_rows, inverse_others))
        ]
    )

    update = -in_order(product(leaf_lower, s_full), product(lower_other, s_full))
    leaf_back = exchange(s_other, 0, 1)
    leaf_solution = in_order(s_mine, leaf_back, 1)

    def gather_z(piece):
        pieces = [piece] + [exchange(piece, 0, m) for m in range(blks - 2, 0, -2)]
        result = jnp.zeros((chips,) + piece.shape, piece.dtype)
        for m, value in zip([0] + list(range(chips - 1, 0, -1)), pieces):
            result = lax.dynamic_update_slice_in_dim(result, value[None], z ^ m, 0)
        return result

    def gather_node(piece, height):
        members = 2**height
        place = k % members
        if members * chips <= DIRECT_LIMIT:
            result = jnp.zeros((members * chips,) + piece.shape, piece.dtype)
            pieces = []
            for a in range(members):
                for m in range(chips):
                    value = piece if a == 0 and m == 0 else exchange(piece, a, 2 * m)
                    pieces.append(((place ^ a) * chips + (z ^ m), value))
            for where, value in pieces:
                result = lax.dynamic_update_slice_in_dim(result, value[None], where, 0)
            return result.reshape(-1, piece.shape[-1])
        joined = piece[None]
        for bit in range(height):
            theirs = exchange(joined, 2**bit, 0)
            upper = (k // 2**bit) % 2 == 1
            joined = jnp.concatenate(
                [jnp.where(upper, theirs, joined), jnp.where(upper, joined, theirs)], axis=0
            )
        return jnp.swapaxes(gather_z(joined), 0, 1).reshape(-1, piece.shape[-1])

    def mix(slot_rows, targets, count):
        result = []
        for t in count:
            hit = (targets == t)[:, :, None, None]
            result.append(jnp.sum(jnp.where(hit, slot_rows, 0), axis=1).reshape(-1, half))
        return result

    def rest_rows(front):
        slots_of = [value.reshape(2, pivots, half) for value in front]
        return jnp.stack(slots_of, axis=1).reshape(-1, half)

    solutions = []
    for height in range(1, levels):
        mask = 2 ** (height - 1)
        offset = base_width * (2**height - 2)
        width = base_width * 2**height
        targets = slots[height - 1]
        slot_rows = update.reshape(2, 2, pivots, half)
        theirs = exchange(slot_rows.astype(dtype), mask, 0).astype(jnp.float32)
        their_targets = their_slots if height == 1 else exchange(targets, mask, 0)
        own = mix(slot_rows, targets, range(3))
        sent = mix(theirs, their_targets, range(3, 6))
        pivot = (seps[height - 1].astype(jnp.float32) + own[0] + sent[0]).astype(dtype)
        rest = rest_rows([own[1] + sent[1], own[2] + sent[2]])
        inverse_here = inv_chip[:, offset : offset + width]
        if height == 1:
            upper = k % 2 == 1

            def by_leaf(near, far):
                return jnp.stack([jnp.where(upper, far, near), jnp.where(upper, near, far)])

            (their_own,) = mix(theirs, their_targets, range(1))
            (their_sent,) = mix(slot_rows, targets, range(3, 4))
            their_pivot = (their_sep.astype(jnp.float32) + their_own + their_sent).astype(dtype)
            pivots_all = gather_z(by_leaf(pivot, their_pivot))
            pivots_all = jnp.swapaxes(pivots_all, 0, 1).reshape(-1, half)
            solved = product(inverse_here, pivots_all).astype(dtype)
            their_solved = product(inv_theirs, pivots_all).astype(dtype)
            solved_all = gather_z(by_leaf(solved, their_solved))
            solved_all = jnp.swapaxes(solved_all, 0, 1).reshape(-1, half)
        else:
            solved = product(inverse_here, gather_node(pivot, height)).astype(dtype)
            solved_all = gather_node(solved, height)
        solutions.append(solved)
        update = rest - product(low_chip[:, offset : offset + width], solved_all)

    own, sent = mix(update.reshape(2, 2, pivots, half), slots[levels - 1], range(2))
    own = own + seps[levels - 1].astype(jnp.float32)
    parts = gather_z(jnp.stack([own, sent]).astype(dtype))
    contributions = jnp.swapaxes(parts, 0, 1).reshape(-1, half)
    partial = product(top_rows, contributions).reshape(leaves, 2 * pivots, half)
    rounded = partial.astype(dtype)
    total = partial[0]
    for a in range(leaves - 1, 0, -1):
        total = total + exchange(rounded[a], a, 0).astype(jnp.float32)
    solutions.append(total.astype(dtype))

    outs = []
    for solved in solutions:
        mine = lax.dynamic_slice_in_dim(solved, core * pivots, pivots, 0)
        other = lax.dynamic_slice_in_dim(solved, (1 - core) * pivots, pivots, 0)
        outs.append(in_order(mine, exchange(other, 0, 1), 1))
    return leaf_solution, jnp.stack(outs)


def solution(mesh):
    return jax.shard_map(
        on_device,
        mesh=mesh,
        in_specs=(
            P(("leaf", "blk"), None),
            P(("leaf", "blk"), None),
            P(("leaf", "blk"), None),
            P(None, ("leaf", "blk"), None),
            P(("leaf", "blk"), None),
            P(("leaf", "blk"), None),
            P(None, ("leaf", "blk"), None),
        ),
        out_specs=(P(("leaf", "blk"), None), P(None, ("leaf", "blk"), None)),
        check_vma=False,
    )
```

```python
import jax
import jax.numpy as jnp
from jax import lax
from jax.experimental import pallas as pl
from jax.experimental.pallas import tpu as pltpu
from jax.sharding import PartitionSpec as P


DIRECT_LIMIT = 16


def exchange(value, leaf_mask, blk_mask):
    leaves = lax.axis_size("leaf")
    blks = lax.axis_size("blk")
    pairs = [
        (k * blks + b, (k ^ leaf_mask) * blks + (b ^ blk_mask))
        for k in range(leaves)
        for b in range(blks)
    ]
    return lax.ppermute(value, ("leaf", "blk"), pairs)


def product(matrix, vectors):
    return jnp.dot(matrix, vectors, preferred_element_type=jnp.float32)


def on_chip(value):
    return pltpu.with_memory_space_constraint(value, pltpu.VMEM)


def vmem_specs(count):
    return [pl.BlockSpec(memory_space=pltpu.VMEM)] * count


def split_masks(blks):
    last = [2, 3, blks - 2, blks - 1]
    return [mask for mask in range(blks) if mask not in last], last


def leaf_partial(pieces, near, far):
    masks = sorted(pieces)
    count = len(masks)
    rows, half = pieces[0].shape
    total = near.shape[1]
    chips = total // (2 * rows)
    dtype = near.dtype

    def body(*refs):
        piece_refs = refs[:count]
        near_ref, far_ref, sum_ref = refs[count : count + 3]
        rests = refs[count + 3 : count + 5]
        rhs, near_vmem, far_vmem, sems = refs[count + 5 :]
        b = lax.axis_index("blk")
        copies = [
            pltpu.make_async_copy(source, target, sems.at[i])
            for i, (source, target) in enumerate(((near_ref, near_vmem), (far_ref, far_vmem)))
        ]
        for copy in copies:
            copy.start()
        missing = [
            pl.multiple_of((b // 2 ^ flip) * 2 * rows, 128) for flip in (1, chips - 1)
        ]
        for where in missing:
            rhs[pl.ds(where, 2 * rows)] = jnp.zeros((2 * rows, half), dtype)
        for mask, piece_ref in zip(masks, piece_refs):
            where = pl.multiple_of((b ^ mask) * rows, 16)
            rhs[pl.ds(where, rows)] = piece_ref[...]
        for i, matrix in enumerate((near_vmem, far_vmem)):
            copies[i].wait()
            sum_ref[i] = jnp.dot(matrix[...], rhs[...], preferred_element_type=jnp.float32)
            for j, where in enumerate(missing):
                columns = pl.ds(j * 2 * rows, 2 * rows)
                rests[i][:, columns] = matrix[:, pl.ds(where, 2 * rows)]

    return pl.pallas_call(
        body,
        in_specs=vmem_specs(count) + [pl.BlockSpec(memory_space=pltpu.HBM)] * 2,
        out_specs=vmem_specs(3),
        out_shape=[
            pltpu.VMEM((2, rows, half), jnp.float32),
            pltpu.VMEM((rows, 4 * rows), dtype),
            pltpu.VMEM((rows, 4 * rows), dtype),
        ],
        scratch_shapes=[
            pltpu.VMEM((total, half), dtype),
            pltpu.VMEM(near.shape, dtype),
            pltpu.VMEM(far.shape, dtype),
            pltpu.SemaphoreType.DMA((2,)),
        ],
        cost_estimate=pl.CostEstimate(
            flops=4 * rows * total * half, bytes_accessed=4 * near.size, transcendentals=0
        ),
        name="leaf_partial",
    )(
        *[on_chip(pieces[mask]) for mask in masks],
        near,
        pltpu.with_memory_space_constraint(far, pltpu.HBM),
    )


def leaf_finish(pieces, sums, rests):
    count = len(pieces)
    rows, half = pieces[0].shape
    dtype = pieces[0].dtype

    def body(*refs):
        piece_refs = refs[:count]
        sum_ref = refs[count]
        rest_refs = refs[count + 1 : count + 3]
        all_ref, mine_ref, other_ref, rhs = refs[count + 3 :]
        core = lax.axis_index("blk") % 2
        for i, piece_ref in enumerate(piece_refs):
            where = pl.multiple_of((i // 2 * 2 + (core ^ i % 2)) * rows, 16)
            rhs[pl.ds(where, rows)] = piece_ref[...]
        for i, out_ref in enumerate((mine_ref, other_ref)):
            value = jnp.dot(rest_refs[i][...], rhs[...], preferred_element_type=jnp.float32)
            value = (value + sum_ref[i]).astype(dtype)
            out_ref[...] = value
            all_ref[pl.ds(pl.multiple_of((core ^ i) * rows, 16), rows)] = value

    return pl.pallas_call(
        body,
        in_specs=vmem_specs(count + 3),
        out_specs=vmem_specs(3),
        out_shape=[
            pltpu.VMEM((2 * rows, half), dtype),
            pltpu.VMEM((rows, half), dtype),
            pltpu.VMEM((rows, half), dtype),
        ],
        scratch_shapes=[pltpu.VMEM((count * rows, half), dtype)],
        cost_estimate=pl.CostEstimate(
            flops=4 * rows * count * rows * half, bytes_accessed=0, transcendentals=0
        ),
        name="leaf_finish",
    )(*[on_chip(value) for value in pieces], on_chip(sums), *[on_chip(value) for value in rests])


def column_halves(value):
    rows, half = value.shape[0], value.shape[1] // 2

    def body(value_ref, own_ref, other_ref, sems):
        core = lax.axis_index("blk") % 2
        copies = []
        for i, out_ref in enumerate((own_ref, other_ref)):
            where = pl.multiple_of((core ^ i) * half, 128)
            copies.append(
                pltpu.make_async_copy(value_ref.at[:, pl.ds(where, half)], out_ref, sems.at[i])
            )
        for copy in copies:
            copy.start()
        for copy in copies:
            copy.wait()

    return pl.pallas_call(
        body,
        in_specs=[pl.BlockSpec(memory_space=pltpu.HBM)],
        out_specs=vmem_specs(2),
        out_shape=[pltpu.VMEM((rows, half), value.dtype)] * 2,
        scratch_shapes=[pltpu.SemaphoreType.DMA((2,))],
        name="column_halves",
    )(value)


def on_device(leaf_rhs, leaf_inverse, leaf_lower, sep_rhs, sep_inverse, sep_lower, slot_map):
    leaves = lax.axis_size("leaf")
    blks = lax.axis_size("blk")
    chips = blks // 2
    k = lax.axis_index("leaf")
    b = lax.axis_index("blk")
    z = b // 2
    core = b % 2
    half = leaf_rhs.shape[1] // 2
    levels, pivots = sep_rhs.shape[0], sep_rhs.shape[1]
    base_width = pivots * blks
    rows = leaf_rhs.shape[0]
    dtype = leaf_rhs.dtype

    def columns_of(value, which):
        return lax.dynamic_slice_in_dim(value, which * half, half, value.ndim - 1)

    def in_order(mine, other, axis=0):
        first = jnp.where(core == 0, mine, other)
        second = jnp.where(core == 0, other, mine)
        return jnp.concatenate([first, second], axis=axis)

    def put(buffer, piece, index):
        return lax.dynamic_update_slice_in_dim(buffer, piece, index * piece.shape[0], 0)

    top_mask = 2 ** (levels - 1)
    top_offset = base_width * (2**levels - 2)
    send_whole = leaves <= DIRECT_LIMIT // 2

    def leaf_columns(value, leaf):
        near = lax.dynamic_slice_in_dim(value, top_offset + leaf * base_width, base_width, 1)
        far = lax.dynamic_slice_in_dim(
            value, top_offset + (leaf ^ top_mask) * base_width, base_width, 1
        )
        return jnp.concatenate([near, far], axis=1)

    inverse_other = exchange(leaf_inverse, 0, 1)
    own_half, other_half = column_halves(leaf_rhs)
    arrived = {0: own_half}
    soon, last = split_masks(blks)
    for mask in soon[:0:-1] + last[::-1]:
        arrived[mask] = exchange(own_half if mask % 2 == 0 else other_half, 0, mask)

    inverse_rows = [sep_inverse]
    for a in range(1, leaves):
        value = sep_inverse
        if not send_whole:
            value = jnp.concatenate([value[:, : 2 * base_width], leaf_columns(value, k ^ a)], 1)
        inverse_rows.append(exchange(value, a, 0))

    pieces = [arrived.pop(mask) for mask in last]
    sums, *beside = leaf_partial(arrived, leaf_inverse, inverse_other)
    s_all, s_mine, s_other = leaf_finish(pieces, sums, beside)
    zorder = [m for m in range(blks - 4, 2, -2)] + [blks - 2, 2]
    got = [(m, exchange(s_all, 0, m)) for m in zorder]
    slot_other = exchange(slot_map, 0, 1)
    sep_rhs_other = exchange(sep_rhs, 0, 1)
    lower_other = exchange(leaf_lower, 0, 1)
    sep_lower_other = exchange(sep_lower, 0, 1)
    s_full = put(jnp.zeros((blks * rows, half), dtype), s_all, z)
    for m, value in got:
        s_full = put(s_full, value, z ^ (m // 2))

    inverse_others = [exchange(value, 0, 1) for value in inverse_rows]
    slots = in_order(slot_map, slot_other, 1)
    seps = in_order(columns_of(sep_rhs, core), columns_of(sep_rhs_other, core), 1)
    paired = levels > 1
    if paired:
        their_slots = exchange(slots[0], 1, 0)
        their_sep = exchange(seps[0], 1, 0)

    low_chip = in_order(sep_lower, sep_lower_other)
    inv_chip = in_order(sep_inverse[:, :top_offset], inverse_others[0][:, :top_offset])
    if paired:
        inv_theirs = in_order(
            inverse_rows[1][:, : 2 * base_width], inverse_others[1][:, : 2 * base_width]
        )

    def top_columns(a, value):
        return leaf_columns(value, k) if a == 0 or send_whole else value[:, 2 * base_width :]

    top_rows = jnp.concatenate(
        [
            in_order(top_columns(a, mine), top_columns(a, other))
            for a, (mine, other) in enumerate(zip(inverse_rows, inverse_others))
        ]
    )

    update = -in_order(product(leaf_lower, s_full), product(lower_other, s_full))
    leaf_back = exchange(s_other, 0, 1)
    leaf_solution = in_order(s_mine, leaf_back, 1)

    def gather_z(piece):
        pieces = [piece] + [exchange(piece, 0, m) for m in range(blks - 2, 0, -2)]
        result = jnp.zeros((chips,) + piece.shape, piece.dtype)
        for m, value in zip([0] + list(range(chips - 1, 0, -1)), pieces):
            result = lax.dynamic_update_slice_in_dim(result, value[None], z ^ m, 0)
        return result

    def gather_node(piece, height):
        members = 2**height
        place = k % members
        if members * chips <= DIRECT_LIMIT:
            result = jnp.zeros((members * chips,) + piece.shape, piece.dtype)
            pieces = []
            for a in range(members):
                for m in range(chips):
                    value = piece if a == 0 and m == 0 else exchange(piece, a, 2 * m)
                    pieces.append(((place ^ a) * chips + (z ^ m), value))
            for where, value in pieces:
                result = lax.dynamic_update_slice_in_dim(result, value[None], where, 0)
            return result.reshape(-1, piece.shape[-1])
        joined = piece[None]
        for bit in range(height):
            theirs = exchange(joined, 2**bit, 0)
            upper = (k // 2**bit) % 2 == 1
            joined = jnp.concatenate(
                [jnp.where(upper, theirs, joined), jnp.where(upper, joined, theirs)], axis=0
            )
        return jnp.swapaxes(gather_z(joined), 0, 1).reshape(-1, piece.shape[-1])

    def mix(slot_rows, targets, count):
        result = []
        for t in count:
            hit = (targets == t)[:, :, None, None]
            result.append(jnp.sum(jnp.where(hit, slot_rows, 0), axis=1).reshape(-1, half))
        return result

    def rest_rows(front):
        slots_of = [value.reshape(2, pivots, half) for value in front]
        return jnp.stack(slots_of, axis=1).reshape(-1, half)

    solutions = []
    for height in range(1, levels):
        mask = 2 ** (height - 1)
        offset = base_width * (2**height - 2)
        width = base_width * 2**height
        targets = slots[height - 1]
        slot_rows = update.reshape(2, 2, pivots, half)
        theirs = exchange(slot_rows.astype(dtype), mask, 0).astype(jnp.float32)
        their_targets = their_slots if height == 1 else exchange(targets, mask, 0)
        own = mix(slot_rows, targets, range(3))
        sent = mix(theirs, their_targets, range(3, 6))
        pivot = (seps[height - 1].astype(jnp.float32) + own[0] + sent[0]).astype(dtype)
        rest = rest_rows([own[1] + sent[1], own[2] + sent[2]])
        inverse_here = inv_chip[:, offset : offset + width]
        if height == 1:
            upper = k % 2 == 1

            def by_leaf(near, far):
                return jnp.stack([jnp.where(upper, far, near), jnp.where(upper, near, far)])

            (their_own,) = mix(theirs, their_targets, range(1))
            (their_sent,) = mix(slot_rows, targets, range(3, 4))
            their_pivot = (their_sep.astype(jnp.float32) + their_own + their_sent).astype(dtype)
            pivots_all = gather_z(by_leaf(pivot, their_pivot))
            pivots_all = jnp.swapaxes(pivots_all, 0, 1).reshape(-1, half)
            solved = product(inverse_here, pivots_all).astype(dtype)
            their_solved = product(inv_theirs, pivots_all).astype(dtype)
            solved_all = gather_z(by_leaf(solved, their_solved))
            solved_all = jnp.swapaxes(solved_all, 0, 1).reshape(-1, half)
        else:
            solved = product(inverse_here, gather_node(pivot, height)).astype(dtype)
            solved_all = gather_node(solved, height)
        solutions.append(solved)
        update = rest - product(low_chip[:, offset : offset + width], solved_all)

    own, sent = mix(update.reshape(2, 2, pivots, half), slots[levels - 1], range(2))
    own = own + seps[levels - 1].astype(jnp.float32)
    parts = gather_z(jnp.stack([own, sent]).astype(dtype))
    contributions = jnp.swapaxes(parts, 0, 1).reshape(-1, half)
    partial = product(top_rows, contributions).reshape(leaves, 2 * pivots, half)
    rounded = partial.astype(dtype)
    total = partial[0]
    for a in range(leaves - 1, 0, -1):
        total = total + exchange(rounded[a], a, 0).astype(jnp.float32)
    solutions.append(total.astype(dtype))

    outs = []
    for solved in solutions:
        mine = lax.dynamic_slice_in_dim(solved, core * pivots, pivots, 0)
        other = lax.dynamic_slice_in_dim(solved, (1 - core) * pivots, pivots, 0)
        outs.append(in_order(mine, exchange(other, 0, 1), 1))
    return leaf_solution, jnp.stack(outs)


def solution(mesh):
    return jax.shard_map(
        on_device,
        mesh=mesh,
        in_specs=(
            P(("leaf", "blk"), None),
            P(("leaf", "blk"), None),
            P(("leaf", "blk"), None),
            P(None, ("leaf", "blk"), None),
            P(("leaf", "blk"), None),
            P(("leaf", "blk"), None),
            P(None, ("leaf", "blk"), None),
        ),
        out_specs=(P(("leaf", "blk"), None), P(None, ("leaf", "blk"), None)),
        check_vma=False,
    )
```

```python
import jax
import jax.numpy as jnp
from jax import lax
from jax.experimental import pallas as pl
from jax.experimental.pallas import tpu as pltpu
from jax.sharding import PartitionSpec as P


DIRECT_LIMIT = 16


def exchange(value, leaf_mask, blk_mask):
    leaves = lax.axis_size("leaf")
    blks = lax.axis_size("blk")
    pairs = [
        (k * blks + b, (k ^ leaf_mask) * blks + (b ^ blk_mask))
        for k in range(leaves)
        for b in range(blks)
    ]
    return lax.ppermute(value, ("leaf", "blk"), pairs)


def product(matrix, vectors):
    return jnp.dot(matrix, vectors, preferred_element_type=jnp.float32)


def on_chip(value):
    return pltpu.with_memory_space_constraint(value, pltpu.VMEM)


def vmem_specs(count):
    return [pl.BlockSpec(memory_space=pltpu.VMEM)] * count


def split_masks(blks):
    last = [2, 3, blks - 2, blks - 1]
    return [mask for mask in range(blks) if mask not in last], last


def leaf_partial(pieces, near, far):
    masks = sorted(pieces)
    count = len(masks)
    rows, half = pieces[0].shape
    total = near.shape[1]
    chips = total // (2 * rows)
    dtype = near.dtype

    def body(*refs):
        piece_refs = refs[:count]
        near_ref, far_ref, sum_ref = refs[count : count + 3]
        rests = refs[count + 3 : count + 5]
        rhs, near_vmem, far_vmem, sems = refs[count + 5 :]
        b = lax.axis_index("blk")
        copies = [
            pltpu.make_async_copy(source, target, sems.at[i])
            for i, (source, target) in enumerate(((near_ref, near_vmem), (far_ref, far_vmem)))
        ]
        for copy in copies:
            copy.start()
        missing = [
            pl.multiple_of((b // 2 ^ flip) * 2 * rows, 128) for flip in (1, chips - 1)
        ]
        for where in missing:
            rhs[pl.ds(where, 2 * rows)] = jnp.zeros((2 * rows, half), dtype)
        for mask, piece_ref in zip(masks, piece_refs):
            where = pl.multiple_of((b ^ mask) * rows, 16)
            rhs[pl.ds(where, rows)] = piece_ref[...]
        for i, matrix in enumerate((near_vmem, far_vmem)):
            copies[i].wait()
            sum_ref[i] = jnp.dot(matrix[...], rhs[...], preferred_element_type=jnp.float32)
            for j, where in enumerate(missing):
                columns = pl.ds(j * 2 * rows, 2 * rows)
                rests[i][:, columns] = matrix[:, pl.ds(where, 2 * rows)]

    return pl.pallas_call(
        body,
        in_specs=vmem_specs(count) + [pl.BlockSpec(memory_space=pltpu.HBM)] * 2,
        out_specs=vmem_specs(3),
        out_shape=[
            pltpu.VMEM((2, rows, half), jnp.float32),
            pltpu.VMEM((rows, 4 * rows), dtype),
            pltpu.VMEM((rows, 4 * rows), dtype),
        ],
        scratch_shapes=[
            pltpu.VMEM((total, half), dtype),
            pltpu.VMEM(near.shape, dtype),
            pltpu.VMEM(far.shape, dtype),
            pltpu.SemaphoreType.DMA((2,)),
        ],
        cost_estimate=pl.CostEstimate(
            flops=4 * rows * total * half, bytes_accessed=4 * near.size, transcendentals=0
        ),
        name="leaf_partial",
    )(
        *[on_chip(pieces[mask]) for mask in masks],
        near,
        pltpu.with_memory_space_constraint(far, pltpu.HBM),
    )


def leaf_finish(pieces, sums, rests):
    count = len(pieces)
    rows, half = pieces[0].shape
    dtype = pieces[0].dtype

    def body(*refs):
        piece_refs = refs[:count]
        sum_ref = refs[count]
        rest_refs = refs[count + 1 : count + 3]
        all_ref, mine_ref, other_ref, rhs = refs[count + 3 :]
        core = lax.axis_index("blk") % 2
        for i, piece_ref in enumerate(piece_refs):
            where = pl.multiple_of((i // 2 * 2 + (core ^ i % 2)) * rows, 16)
            rhs[pl.ds(where, rows)] = piece_ref[...]
        for i, out_ref in enumerate((mine_ref, other_ref)):
            value = jnp.dot(rest_refs[i][...], rhs[...], preferred_element_type=jnp.float32)
            value = (value + sum_ref[i]).astype(dtype)
            out_ref[...] = value
            all_ref[pl.ds(pl.multiple_of((core ^ i) * rows, 16), rows)] = value

    return pl.pallas_call(
        body,
        in_specs=vmem_specs(count + 3),
        out_specs=vmem_specs(3),
        out_shape=[
            pltpu.VMEM((2 * rows, half), dtype),
            pltpu.VMEM((rows, half), dtype),
            pltpu.VMEM((rows, half), dtype),
        ],
        scratch_shapes=[pltpu.VMEM((count * rows, half), dtype)],
        cost_estimate=pl.CostEstimate(
            flops=4 * rows * count * rows * half, bytes_accessed=0, transcendentals=0
        ),
        name="leaf_finish",
    )(*[on_chip(value) for value in pieces], on_chip(sums), *[on_chip(value) for value in rests])


def column_halves(value):
    rows, half = value.shape[0], value.shape[1] // 2

    def body(value_ref, own_ref, other_ref, sems):
        core = lax.axis_index("blk") % 2
        copies = []
        for i, out_ref in enumerate((own_ref, other_ref)):
            where = pl.multiple_of((core ^ i) * half, 128)
            copies.append(
                pltpu.make_async_copy(value_ref.at[:, pl.ds(where, half)], out_ref, sems.at[i])
            )
        for copy in copies:
            copy.start()
        for copy in copies:
            copy.wait()

    return pl.pallas_call(
        body,
        in_specs=[pl.BlockSpec(memory_space=pltpu.HBM)],
        out_specs=vmem_specs(2),
        out_shape=[pltpu.VMEM((rows, half), value.dtype)] * 2,
        scratch_shapes=[pltpu.SemaphoreType.DMA((2,))],
        name="column_halves",
    )(value)


def on_device(leaf_rhs, leaf_inverse, leaf_lower, sep_rhs, sep_inverse, sep_lower, slot_map):
    leaves = lax.axis_size("leaf")
    blks = lax.axis_size("blk")
    chips = blks // 2
    k = lax.axis_index("leaf")
    b = lax.axis_index("blk")
    z = b // 2
    core = b % 2
    half = leaf_rhs.shape[1] // 2
    levels, pivots = sep_rhs.shape[0], sep_rhs.shape[1]
    base_width = pivots * blks
    rows = leaf_rhs.shape[0]
    dtype = leaf_rhs.dtype

    def columns_of(value, which):
        return lax.dynamic_slice_in_dim(value, which * half, half, value.ndim - 1)

    def in_order(mine, other, axis=0):
        first = jnp.where(core == 0, mine, other)
        second = jnp.where(core == 0, other, mine)
        return jnp.concatenate([first, second], axis=axis)

    def put(buffer, piece, index):
        return lax.dynamic_update_slice_in_dim(buffer, piece, index * piece.shape[0], 0)

    top_mask = 2 ** (levels - 1)
    top_offset = base_width * (2**levels - 2)
    send_whole = leaves <= DIRECT_LIMIT // 2

    def leaf_columns(value, leaf):
        near = lax.dynamic_slice_in_dim(value, top_offset + leaf * base_width, base_width, 1)
        far = lax.dynamic_slice_in_dim(
            value, top_offset + (leaf ^ top_mask) * base_width, base_width, 1
        )
        return jnp.concatenate([near, far], axis=1)

    inverse_other = exchange(leaf_inverse, 0, 1)
    own_half, other_half = column_halves(leaf_rhs)
    arrived = {0: own_half}
    soon, last = split_masks(blks)
    for mask in soon[:0:-1] + last[::-1]:
        arrived[mask] = exchange(own_half if mask % 2 == 0 else other_half, 0, mask)

    inverse_rows = [sep_inverse]
    for a in range(1, leaves):
        value = sep_inverse
        if not send_whole:
            value = jnp.concatenate([value[:, : 2 * base_width], leaf_columns(value, k ^ a)], 1)
        inverse_rows.append(exchange(value, a, 0))

    pieces = [arrived.pop(mask) for mask in last]
    sums, *beside = leaf_partial(arrived, leaf_inverse, inverse_other)
    s_all, s_mine, s_other = leaf_finish(pieces, sums, beside)
    zorder = [m for m in range(blks - 4, 2, -2)] + [blks - 2, 2]
    got = [(m, exchange(s_all, 0, m)) for m in zorder]
    slot_other = exchange(slot_map, 0, 1)
    sep_rhs_other = exchange(sep_rhs, 0, 1)
    lower_other = exchange(leaf_lower, 0, 1)
    sep_lower_other = exchange(sep_lower, 0, 1)
    s_full = put(jnp.zeros((blks * rows, half), dtype), s_all, z)
    for m, value in got:
        s_full = put(s_full, value, z ^ (m // 2))

    inverse_others = [exchange(value, 0, 1) for value in inverse_rows]
    slots = in_order(slot_map, slot_other, 1)
    seps = in_order(columns_of(sep_rhs, core), columns_of(sep_rhs_other, core), 1)
    paired = levels > 1
    if paired:
        their_slots = exchange(slots[0], 1, 0)
        their_sep = exchange(seps[0], 1, 0)

    low_chip = in_order(sep_lower, sep_lower_other)
    inv_chip = in_order(sep_inverse[:, :top_offset], inverse_others[0][:, :top_offset])
    if paired:
        inv_own, inv_theirs = [
            in_order(mine[:, : 2 * base_width], other[:, : 2 * base_width])
            for mine, other in zip(inverse_rows[:2], inverse_others[:2])
        ]
        inv_pair = jnp.concatenate(
            [jnp.where(k % 2 == 1, inv_theirs, inv_own), jnp.where(k % 2 == 1, inv_own, inv_theirs)]
        )

    def top_columns(a, value):
        return leaf_columns(value, k) if a == 0 or send_whole else value[:, 2 * base_width :]

    top_rows = jnp.concatenate(
        [
            in_order(top_columns(a, mine), top_columns(a, other))
            for a, (mine, other) in enumerate(zip(inverse_rows, inverse_others))
        ]
    )

    update = -in_order(product(leaf_lower, s_full), product(lower_other, s_full))
    leaf_back = exchange(s_other, 0, 1)
    leaf_solution = in_order(s_mine, leaf_back, 1)

    def gather_z(piece):
        pieces = [piece] + [exchange(piece, 0, m) for m in range(blks - 2, 0, -2)]
        result = jnp.zeros((chips,) + piece.shape, piece.dtype)
        for m, value in zip([0] + list(range(chips - 1, 0, -1)), pieces):
            result = lax.dynamic_update_slice_in_dim(result, value[None], z ^ m, 0)
        return result

    def gather_node(piece, height):
        members = 2**height
        place = k % members
        if members * chips <= DIRECT_LIMIT:
            result = jnp.zeros((members * chips,) + piece.shape, piece.dtype)
            pieces = []
            for a in range(members):
                for m in range(chips):
                    value = piece if a == 0 and m == 0 else exchange(piece, a, 2 * m)
                    pieces.append(((place ^ a) * chips + (z ^ m), value))
            for where, value in pieces:
                result = lax.dynamic_update_slice_in_dim(result, value[None], where, 0)
            return result.reshape(-1, piece.shape[-1])
        joined = piece[None]
        for bit in range(height):
            theirs = exchange(joined, 2**bit, 0)
            upper = (k // 2**bit) % 2 == 1
            joined = jnp.concatenate(
                [jnp.where(upper, theirs, joined), jnp.where(upper, joined, theirs)], axis=0
            )
        return jnp.swapaxes(gather_z(joined), 0, 1).reshape(-1, piece.shape[-1])

    def mix(slot_rows, targets, count):
        result = []
        for t in count:
            hit = (targets == t)[:, :, None, None]
            result.append(jnp.sum(jnp.where(hit, slot_rows, 0), axis=1).reshape(-1, half))
        return result

    def rest_rows(front):
        slots_of = [value.reshape(2, pivots, half) for value in front]
        return jnp.stack(slots_of, axis=1).reshape(-1, half)

    solutions = []
    for height in range(1, levels):
        mask = 2 ** (height - 1)
        offset = base_width * (2**height - 2)
        width = base_width * 2**height
        targets = slots[height - 1]
        slot_rows = update.reshape(2, 2, pivots, half)
        theirs = exchange(slot_rows.astype(dtype), mask, 0).astype(jnp.float32)
        their_targets = their_slots if height == 1 else exchange(targets, mask, 0)
        own = mix(slot_rows, targets, range(3))
        sent = mix(theirs, their_targets, range(3, 6))
        pivot = (seps[height - 1].astype(jnp.float32) + own[0] + sent[0]).astype(dtype)
        rest = rest_rows([own[1] + sent[1], own[2] + sent[2]])
        inverse_here = inv_chip[:, offset : offset + width]
        if height == 1:
            upper = k % 2 == 1

            def by_leaf(near, far):
                return jnp.stack([jnp.where(upper, far, near), jnp.where(upper, near, far)])

            (their_own,) = mix(theirs, their_targets, range(1))
            (their_sent,) = mix(slot_rows, targets, range(3, 4))
            their_pivot = (their_sep.astype(jnp.float32) + their_own + their_sent).astype(dtype)
            pivots_all = gather_z(by_leaf(pivot, their_pivot))
            pivots_all = jnp.swapaxes(pivots_all, 0, 1).reshape(-1, half)
            both = product(inv_pair, pivots_all).astype(dtype)
            solved = lax.dynamic_slice_in_dim(both, k % 2 * 2 * pivots, 2 * pivots, 0)
            solved_all = gather_z(both.reshape(2, 2 * pivots, half))
            solved_all = jnp.swapaxes(solved_all, 0, 1).reshape(-1, half)
        else:
            solved = product(inverse_here, gather_node(pivot, height)).astype(dtype)
            solved_all = gather_node(solved, height)
        solutions.append(solved)
        update = rest - product(low_chip[:, offset : offset + width], solved_all)

    own, sent = mix(update.reshape(2, 2, pivots, half), slots[levels - 1], range(2))
    own = own + seps[levels - 1].astype(jnp.float32)
    parts = gather_z(jnp.stack([own, sent]).astype(dtype))
    contributions = jnp.swapaxes(parts, 0, 1).reshape(-1, half)
    partial = product(top_rows, contributions).reshape(leaves, 2 * pivots, half)
    rounded = partial.astype(dtype)
    total = partial[0]
    for a in range(leaves - 1, 0, -1):
        total = total + exchange(rounded[a], a, 0).astype(jnp.float32)
    solutions.append(total.astype(dtype))

    outs = []
    for solved in solutions:
        mine = lax.dynamic_slice_in_dim(solved, core * pivots, pivots, 0)
        other = lax.dynamic_slice_in_dim(solved, (1 - core) * pivots, pivots, 0)
        outs.append(in_order(mine, exchange(other, 0, 1), 1))
    return leaf_solution, jnp.stack(outs)


def solution(mesh):
    return jax.shard_map(
        on_device,
        mesh=mesh,
        in_specs=(
            P(("leaf", "blk"), None),
            P(("leaf", "blk"), None),
            P(("leaf", "blk"), None),
            P(None, ("leaf", "blk"), None),
            P(("leaf", "blk"), None),
            P(("leaf", "blk"), None),
            P(None, ("leaf", "blk"), None),
        ),
        out_specs=(P(("leaf", "blk"), None), P(None, ("leaf", "blk"), None)),
        check_vma=False,
    )
```

```python
import jax
import jax.numpy as jnp
from jax import lax
from jax.experimental import pallas as pl
from jax.experimental.pallas import tpu as pltpu
from jax.sharding import PartitionSpec as P


DIRECT_LIMIT = 16


def exchange(value, leaf_mask, blk_mask):
    leaves = lax.axis_size("leaf")
    blks = lax.axis_size("blk")
    pairs = [
        (k * blks + b, (k ^ leaf_mask) * blks + (b ^ blk_mask))
        for k in range(leaves)
        for b in range(blks)
    ]
    return lax.ppermute(value, ("leaf", "blk"), pairs)


def product(matrix, vectors):
    return jnp.dot(matrix, vectors, preferred_element_type=jnp.float32)


def on_chip(value):
    return pltpu.with_memory_space_constraint(value, pltpu.VMEM)


def vmem_specs(count):
    return [pl.BlockSpec(memory_space=pltpu.VMEM)] * count


def split_masks(blks):
    last = [2, 3, blks - 2, blks - 1]
    return [mask for mask in range(blks) if mask not in last], last


def leaf_partial(pieces, near, far):
    masks = sorted(pieces)
    count = len(masks)
    rows, half = pieces[0].shape
    total = near.shape[1]
    chips = total // (2 * rows)
    dtype = near.dtype

    def body(*refs):
        piece_refs = refs[:count]
        near_ref, far_ref, sum_ref = refs[count : count + 3]
        rests = refs[count + 3 : count + 5]
        rhs, near_vmem, far_vmem, sems = refs[count + 5 :]
        b = lax.axis_index("blk")
        copies = [
            pltpu.make_async_copy(source, target, sems.at[i])
            for i, (source, target) in enumerate(((near_ref, near_vmem), (far_ref, far_vmem)))
        ]
        for copy in copies:
            copy.start()
        missing = [
            pl.multiple_of((b // 2 ^ flip) * 2 * rows, 128) for flip in (1, chips - 1)
        ]
        for where in missing:
            rhs[pl.ds(where, 2 * rows)] = jnp.zeros((2 * rows, half), dtype)
        for mask, piece_ref in zip(masks, piece_refs):
            where = pl.multiple_of((b ^ mask) * rows, 16)
            rhs[pl.ds(where, rows)] = piece_ref[...]
        for i, matrix in enumerate((near_vmem, far_vmem)):
            copies[i].wait()
            sum_ref[i] = jnp.dot(matrix[...], rhs[...], preferred_element_type=jnp.float32)
            for j, where in enumerate(missing):
                columns = pl.ds(j * 2 * rows, 2 * rows)
                rests[i][:, columns] = matrix[:, pl.ds(where, 2 * rows)]

    return pl.pallas_call(
        body,
        in_specs=vmem_specs(count) + [pl.BlockSpec(memory_space=pltpu.HBM)] * 2,
        out_specs=vmem_specs(3),
        out_shape=[
            pltpu.VMEM((2, rows, half), jnp.float32),
            pltpu.VMEM((rows, 4 * rows), dtype),
            pltpu.VMEM((rows, 4 * rows), dtype),
        ],
        scratch_shapes=[
            pltpu.VMEM((total, half), dtype),
            pltpu.VMEM(near.shape, dtype),
            pltpu.VMEM(far.shape, dtype),
            pltpu.SemaphoreType.DMA((2,)),
        ],
        cost_estimate=pl.CostEstimate(
            flops=4 * rows * total * half, bytes_accessed=4 * near.size, transcendentals=0
        ),
        name="leaf_partial",
    )(
        *[on_chip(pieces[mask]) for mask in masks],
        near,
        pltpu.with_memory_space_constraint(far, pltpu.HBM),
    )


def leaf_finish(pieces, sums, rests):
    count = len(pieces)
    rows, half = pieces[0].shape
    dtype = pieces[0].dtype

    def body(*refs):
        piece_refs = refs[:count]
        sum_ref = refs[count]
        rest_refs = refs[count + 1 : count + 3]
        all_ref, mine_ref, other_ref, rhs = refs[count + 3 :]
        core = lax.axis_index("blk") % 2
        for i, piece_ref in enumerate(piece_refs):
            where = pl.multiple_of((i // 2 * 2 + (core ^ i % 2)) * rows, 16)
            rhs[pl.ds(where, rows)] = piece_ref[...]
        for i, out_ref in enumerate((mine_ref, other_ref)):
            value = jnp.dot(rest_refs[i][...], rhs[...], preferred_element_type=jnp.float32)
            value = (value + sum_ref[i]).astype(dtype)
            out_ref[...] = value
            all_ref[pl.ds(pl.multiple_of((core ^ i) * rows, 16), rows)] = value

    return pl.pallas_call(
        body,
        in_specs=vmem_specs(count + 3),
        out_specs=vmem_specs(3),
        out_shape=[
            pltpu.VMEM((2 * rows, half), dtype),
            pltpu.VMEM((rows, half), dtype),
            pltpu.VMEM((rows, half), dtype),
        ],
        scratch_shapes=[pltpu.VMEM((count * rows, half), dtype)],
        cost_estimate=pl.CostEstimate(
            flops=4 * rows * count * rows * half, bytes_accessed=0, transcendentals=0
        ),
        name="leaf_finish",
    )(*[on_chip(value) for value in pieces], on_chip(sums), *[on_chip(value) for value in rests])


def column_halves(value):
    rows, half = value.shape[0], value.shape[1] // 2

    def body(value_ref, own_ref, other_ref, sems):
        core = lax.axis_index("blk") % 2
        copies = []
        for i, out_ref in enumerate((own_ref, other_ref)):
            where = pl.multiple_of((core ^ i) * half, 128)
            copies.append(
                pltpu.make_async_copy(value_ref.at[:, pl.ds(where, half)], out_ref, sems.at[i])
            )
        for copy in copies:
            copy.start()
        for copy in copies:
            copy.wait()

    return pl.pallas_call(
        body,
        in_specs=[pl.BlockSpec(memory_space=pltpu.HBM)],
        out_specs=vmem_specs(2),
        out_shape=[pltpu.VMEM((rows, half), value.dtype)] * 2,
        scratch_shapes=[pltpu.SemaphoreType.DMA((2,))],
        name="column_halves",
    )(value)


def on_device(leaf_rhs, leaf_inverse, leaf_lower, sep_rhs, sep_inverse, sep_lower, slot_map):
    leaves = lax.axis_size("leaf")
    blks = lax.axis_size("blk")
    chips = blks // 2
    k = lax.axis_index("leaf")
    b = lax.axis_index("blk")
    z = b // 2
    core = b % 2
    half = leaf_rhs.shape[1] // 2
    levels, pivots = sep_rhs.shape[0], sep_rhs.shape[1]
    base_width = pivots * blks
    rows = leaf_rhs.shape[0]
    dtype = leaf_rhs.dtype

    def columns_of(value, which):
        return lax.dynamic_slice_in_dim(value, which * half, half, value.ndim - 1)

    def in_order(mine, other, axis=0):
        first = jnp.where(core == 0, mine, other)
        second = jnp.where(core == 0, other, mine)
        return jnp.concatenate([first, second], axis=axis)

    def put(buffer, piece, index):
        return lax.dynamic_update_slice_in_dim(buffer, piece, index * piece.shape[0], 0)

    top_mask = 2 ** (levels - 1)
    top_offset = base_width * (2**levels - 2)
    send_whole = leaves <= DIRECT_LIMIT // 2

    def leaf_columns(value, leaf):
        near = lax.dynamic_slice_in_dim(value, top_offset + leaf * base_width, base_width, 1)
        far = lax.dynamic_slice_in_dim(
            value, top_offset + (leaf ^ top_mask) * base_width, base_width, 1
        )
        return jnp.concatenate([near, far], axis=1)

    inverse_other = exchange(leaf_inverse, 0, 1)
    own_half, other_half = column_halves(leaf_rhs)
    arrived = {0: own_half}
    soon, last = split_masks(blks)
    for mask in soon[:0:-1] + last[::-1]:
        arrived[mask] = exchange(own_half if mask % 2 == 0 else other_half, 0, mask)

    inverse_rows = [sep_inverse]
    for a in range(1, leaves):
        value = sep_inverse
        if not send_whole:
            value = jnp.concatenate([value[:, : 2 * base_width], leaf_columns(value, k ^ a)], 1)
        inverse_rows.append(exchange(value, a, 0))

    pieces = [arrived.pop(mask) for mask in last]
    sums, *beside = leaf_partial(arrived, leaf_inverse, inverse_other)
    s_all, s_mine, s_other = leaf_finish(pieces, sums, beside)
    zorder = [m for m in range(blks - 4, 2, -2)] + [blks - 2, 2]
    got = [(m, exchange(s_all, 0, m)) for m in zorder]
    slot_other = exchange(slot_map, 0, 1)
    sep_rhs_other = exchange(sep_rhs, 0, 1)
    lower_other = exchange(leaf_lower, 0, 1)
    sep_lower_other = exchange(sep_lower, 0, 1)
    s_full = put(jnp.zeros((blks * rows, half), dtype), s_all, z)
    for m, value in got:
        s_full = put(s_full, value, z ^ (m // 2))

    inverse_others = [exchange(value, 0, 1) for value in inverse_rows]
    slots = in_order(slot_map, slot_other, 1)
    seps = in_order(columns_of(sep_rhs, core), columns_of(sep_rhs_other, core), 1)
    paired = levels > 1
    if paired:
        their_slots = exchange(slots[0], 1, 0)
        their_sep = exchange(seps[0], 1, 0)

    low_chip = in_order(sep_lower, sep_lower_other)
    inv_chip = in_order(sep_inverse[:, :top_offset], inverse_others[0][:, :top_offset])
    if paired:
        inv_own, inv_theirs = [
            in_order(mine[:, : 2 * base_width], other[:, : 2 * base_width])
            for mine, other in zip(inverse_rows[:2], inverse_others[:2])
        ]
        inv_pair = jnp.concatenate(
            [jnp.where(k % 2 == 1, inv_theirs, inv_own), jnp.where(k % 2 == 1, inv_own, inv_theirs)]
        )

    def top_columns(a, value):
        return leaf_columns(value, k) if a == 0 or send_whole else value[:, 2 * base_width :]

    top_blocks = []
    for a, (mine, other) in enumerate(zip(inverse_rows, inverse_others)):
        top_blocks.append(in_order(top_columns(a, mine), top_columns(a, other)))
    top_rows = jnp.concatenate(top_blocks)

    update = -in_order(product(leaf_lower, s_full), product(lower_other, s_full))
    leaf_back = exchange(s_other, 0, 1)
    leaf_solution = in_order(s_mine, leaf_back, 1)

    def gather_z(piece):
        pieces = [piece] + [exchange(piece, 0, m) for m in range(blks - 2, 0, -2)]
        result = jnp.zeros((chips,) + piece.shape, piece.dtype)
        for m, value in zip([0] + list(range(chips - 1, 0, -1)), pieces):
            result = lax.dynamic_update_slice_in_dim(result, value[None], z ^ m, 0)
        return result

    def gather_node(piece, height):
        members = 2**height
        place = k % members
        if members * chips <= DIRECT_LIMIT:
            result = jnp.zeros((members * chips,) + piece.shape, piece.dtype)
            pieces = []
            for a in range(members):
                for m in range(chips):
                    value = piece if a == 0 and m == 0 else exchange(piece, a, 2 * m)
                    pieces.append(((place ^ a) * chips + (z ^ m), value))
            for where, value in pieces:
                result = lax.dynamic_update_slice_in_dim(result, value[None], where, 0)
            return result.reshape(-1, piece.shape[-1])
        joined = piece[None]
        for bit in range(height):
            theirs = exchange(joined, 2**bit, 0)
            upper = (k // 2**bit) % 2 == 1
            joined = jnp.concatenate(
                [jnp.where(upper, theirs, joined), jnp.where(upper, joined, theirs)], axis=0
            )
        return jnp.swapaxes(gather_z(joined), 0, 1).reshape(-1, piece.shape[-1])

    def mix(slot_rows, targets, count):
        result = []
        for t in count:
            hit = (targets == t)[:, :, None, None]
            result.append(jnp.sum(jnp.where(hit, slot_rows, 0), axis=1).reshape(-1, half))
        return result

    def rest_rows(front):
        slots_of = [value.reshape(2, pivots, half) for value in front]
        return jnp.stack(slots_of, axis=1).reshape(-1, half)

    solutions = []
    for height in range(1, levels):
        mask = 2 ** (height - 1)
        offset = base_width * (2**height - 2)
        width = base_width * 2**height
        targets = slots[height - 1]
        slot_rows = update.reshape(2, 2, pivots, half)
        theirs = exchange(slot_rows.astype(dtype), mask, 0).astype(jnp.float32)
        their_targets = their_slots if height == 1 else exchange(targets, mask, 0)
        own = mix(slot_rows, targets, range(3))
        sent = mix(theirs, their_targets, range(3, 6))
        pivot = (seps[height - 1].astype(jnp.float32) + own[0] + sent[0]).astype(dtype)
        rest = rest_rows([own[1] + sent[1], own[2] + sent[2]])
        inverse_here = inv_chip[:, offset : offset + width]
        if height == 1:
            upper = k % 2 == 1

            def by_leaf(near, far):
                return jnp.stack([jnp.where(upper, far, near), jnp.where(upper, near, far)])

            (their_own,) = mix(theirs, their_targets, range(1))
            (their_sent,) = mix(slot_rows, targets, range(3, 4))
            their_pivot = (their_sep.astype(jnp.float32) + their_own + their_sent).astype(dtype)
            pivots_all = gather_z(by_leaf(pivot, their_pivot))
            pivots_all = jnp.swapaxes(pivots_all, 0, 1).reshape(-1, half)
            both = product(inv_pair, pivots_all).astype(dtype)
            solved = lax.dynamic_slice_in_dim(both, k % 2 * 2 * pivots, 2 * pivots, 0)
            solved_all = gather_z(both.reshape(2, 2 * pivots, half))
            solved_all = jnp.swapaxes(solved_all, 0, 1).reshape(-1, half)
        else:
            solved = product(inverse_here, gather_node(pivot, height)).astype(dtype)
            solved_all = gather_node(solved, height)
        solutions.append(solved)
        update = rest - product(low_chip[:, offset : offset + width], solved_all)

    own, sent = mix(update.reshape(2, 2, pivots, half), slots[levels - 1], range(2))
    own = own + seps[levels - 1].astype(jnp.float32)
    parts = gather_z(jnp.stack([own, sent]).astype(dtype))
    contributions = jnp.swapaxes(parts, 0, 1).reshape(-1, half)
    partial = product(top_rows, contributions).reshape(leaves, 2 * pivots, half)
    rounded = partial.astype(dtype)
    total = partial[0]
    for a in range(leaves - 1, 0, -1):
        total = total + exchange(rounded[a], a, 0).astype(jnp.float32)
    solutions.append(total.astype(dtype))

    outs = []
    for solved in solutions:
        mine = lax.dynamic_slice_in_dim(solved, core * pivots, pivots, 0)
        other = lax.dynamic_slice_in_dim(solved, (1 - core) * pivots, pivots, 0)
        outs.append(in_order(mine, exchange(other, 0, 1), 1))
    return leaf_solution, jnp.stack(outs)


def solution(mesh):
    return jax.shard_map(
        on_device,
        mesh=mesh,
        in_specs=(
            P(("leaf", "blk"), None),
            P(("leaf", "blk"), None),
            P(("leaf", "blk"), None),
            P(None, ("leaf", "blk"), None),
            P(("leaf", "blk"), None),
            P(("leaf", "blk"), None),
            P(None, ("leaf", "blk"), None),
        ),
        out_specs=(P(("leaf", "blk"), None), P(None, ("leaf", "blk"), None)),
        check_vma=False,
    )
```

```python
import jax
import jax.numpy as jnp
from jax import lax
from jax.experimental import pallas as pl
from jax.experimental.pallas import tpu as pltpu
from jax.sharding import PartitionSpec as P


DIRECT_LIMIT = 16


def exchange(value, leaf_mask, blk_mask):
    leaves = lax.axis_size("leaf")
    blks = lax.axis_size("blk")
    pairs = [
        (k * blks + b, (k ^ leaf_mask) * blks + (b ^ blk_mask))
        for k in range(leaves)
        for b in range(blks)
    ]
    return lax.ppermute(value, ("leaf", "blk"), pairs)


def product(matrix, vectors):
    return jnp.dot(matrix, vectors, preferred_element_type=jnp.float32)


def on_chip(value):
    return pltpu.with_memory_space_constraint(value, pltpu.VMEM)


def vmem_specs(count):
    return [pl.BlockSpec(memory_space=pltpu.VMEM)] * count


def split_masks(blks):
    last = [2, 3, blks - 2, blks - 1]
    return [mask for mask in range(blks) if mask not in last], last


def leaf_partial(pieces, near, far):
    masks = sorted(pieces)
    count = len(masks)
    rows, half = pieces[0].shape
    total = near.shape[1]
    chips = total // (2 * rows)
    dtype = near.dtype

    def body(*refs):
        piece_refs = refs[:count]
        near_ref, far_ref, sum_ref = refs[count : count + 3]
        rests = refs[count + 3 : count + 5]
        rhs, near_vmem, far_vmem, sems = refs[count + 5 :]
        b = lax.axis_index("blk")
        copies = [
            pltpu.make_async_copy(source, target, sems.at[i])
            for i, (source, target) in enumerate(((near_ref, near_vmem), (far_ref, far_vmem)))
        ]
        for copy in copies:
            copy.start()
        missing = [
            pl.multiple_of((b // 2 ^ flip) * 2 * rows, 128) for flip in (1, chips - 1)
        ]
        for where in missing:
            rhs[pl.ds(where, 2 * rows)] = jnp.zeros((2 * rows, half), dtype)
        for mask, piece_ref in zip(masks, piece_refs):
            where = pl.multiple_of((b ^ mask) * rows, 16)
            rhs[pl.ds(where, rows)] = piece_ref[...]
        for i, matrix in enumerate((near_vmem, far_vmem)):
            copies[i].wait()
            sum_ref[i] = jnp.dot(matrix[...], rhs[...], preferred_element_type=jnp.float32)
            for j, where in enumerate(missing):
                columns = pl.ds(j * 2 * rows, 2 * rows)
                rests[i][:, columns] = matrix[:, pl.ds(where, 2 * rows)]

    return pl.pallas_call(
        body,
        in_specs=vmem_specs(count) + [pl.BlockSpec(memory_space=pltpu.HBM)] * 2,
        out_specs=vmem_specs(3),
        out_shape=[
            pltpu.VMEM((2, rows, half), jnp.float32),
            pltpu.VMEM((rows, 4 * rows), dtype),
            pltpu.VMEM((rows, 4 * rows), dtype),
        ],
        scratch_shapes=[
            pltpu.VMEM((total, half), dtype),
            pltpu.VMEM(near.shape, dtype),
            pltpu.VMEM(far.shape, dtype),
            pltpu.SemaphoreType.DMA((2,)),
        ],
        cost_estimate=pl.CostEstimate(
            flops=4 * rows * total * half, bytes_accessed=4 * near.size, transcendentals=0
        ),
        name="leaf_partial",
    )(
        *[on_chip(pieces[mask]) for mask in masks],
        near,
        pltpu.with_memory_space_constraint(far, pltpu.HBM),
    )


def leaf_finish(pieces, sums, rests):
    count = len(pieces)
    rows, half = pieces[0].shape
    dtype = pieces[0].dtype

    def body(*refs):
        piece_refs = refs[:count]
        sum_ref = refs[count]
        rest_refs = refs[count + 1 : count + 3]
        all_ref, mine_ref, other_ref, rhs = refs[count + 3 :]
        core = lax.axis_index("blk") % 2
        for i, piece_ref in enumerate(piece_refs):
            where = pl.multiple_of((i // 2 * 2 + (core ^ i % 2)) * rows, 16)
            rhs[pl.ds(where, rows)] = piece_ref[...]
        for i, out_ref in enumerate((mine_ref, other_ref)):
            value = jnp.dot(rest_refs[i][...], rhs[...], preferred_element_type=jnp.float32)
            value = (value + sum_ref[i]).astype(dtype)
            out_ref[...] = value
            all_ref[pl.ds(pl.multiple_of((core ^ i) * rows, 16), rows)] = value

    return pl.pallas_call(
        body,
        in_specs=vmem_specs(count + 3),
        out_specs=vmem_specs(3),
        out_shape=[
            pltpu.VMEM((2 * rows, half), dtype),
            pltpu.VMEM((rows, half), dtype),
            pltpu.VMEM((rows, half), dtype),
        ],
        scratch_shapes=[pltpu.VMEM((count * rows, half), dtype)],
        cost_estimate=pl.CostEstimate(
            flops=4 * rows * count * rows * half, bytes_accessed=0, transcendentals=0
        ),
        name="leaf_finish",
    )(*[on_chip(value) for value in pieces], on_chip(sums), *[on_chip(value) for value in rests])


def column_halves(value):
    rows, half = value.shape[0], value.shape[1] // 2

    def body(value_ref, own_ref, other_ref, sems):
        core = lax.axis_index("blk") % 2
        copies = []
        for i, out_ref in enumerate((own_ref, other_ref)):
            where = pl.multiple_of((core ^ i) * half, 128)
            copies.append(
                pltpu.make_async_copy(value_ref.at[:, pl.ds(where, half)], out_ref, sems.at[i])
            )
        for copy in copies:
            copy.start()
        for copy in copies:
            copy.wait()

    return pl.pallas_call(
        body,
        in_specs=[pl.BlockSpec(memory_space=pltpu.HBM)],
        out_specs=vmem_specs(2),
        out_shape=[pltpu.VMEM((rows, half), value.dtype)] * 2,
        scratch_shapes=[pltpu.SemaphoreType.DMA((2,))],
        name="column_halves",
    )(value)


def on_device(leaf_rhs, leaf_inverse, leaf_lower, sep_rhs, sep_inverse, sep_lower, slot_map):
    leaves = lax.axis_size("leaf")
    blks = lax.axis_size("blk")
    chips = blks // 2
    k = lax.axis_index("leaf")
    b = lax.axis_index("blk")
    z = b // 2
    core = b % 2
    half = leaf_rhs.shape[1] // 2
    levels, pivots = sep_rhs.shape[0], sep_rhs.shape[1]
    base_width = pivots * blks
    rows = leaf_rhs.shape[0]
    dtype = leaf_rhs.dtype

    def columns_of(value, which):
        return lax.dynamic_slice_in_dim(value, which * half, half, value.ndim - 1)

    def in_order(mine, other, axis=0):
        first = jnp.where(core == 0, mine, other)
        second = jnp.where(core == 0, other, mine)
        return jnp.concatenate([first, second], axis=axis)

    def put(buffer, piece, index):
        return lax.dynamic_update_slice_in_dim(buffer, piece, index * piece.shape[0], 0)

    top_mask = 2 ** (levels - 1)
    top_offset = base_width * (2**levels - 2)
    send_whole = leaves <= DIRECT_LIMIT // 2

    def leaf_columns(value, leaf):
        near = lax.dynamic_slice_in_dim(value, top_offset + leaf * base_width, base_width, 1)
        far = lax.dynamic_slice_in_dim(
            value, top_offset + (leaf ^ top_mask) * base_width, base_width, 1
        )
        return jnp.concatenate([near, far], axis=1)

    inverse_other = exchange(leaf_inverse, 0, 1)
    own_half, other_half = column_halves(leaf_rhs)
    arrived = {0: own_half}
    soon, last = split_masks(blks)
    for mask in soon[:0:-1] + last[::-1]:
        arrived[mask] = exchange(own_half if mask % 2 == 0 else other_half, 0, mask)

    inverse_rows = [sep_inverse]
    for a in range(1, leaves):
        value = sep_inverse
        if not send_whole:
            value = jnp.concatenate([value[:, : 2 * base_width], leaf_columns(value, k ^ a)], 1)
        inverse_rows.append(exchange(value, a, 0))

    pieces = [arrived.pop(mask) for mask in last]
    sums, *beside = leaf_partial(arrived, leaf_inverse, inverse_other)
    s_all, s_mine, s_other = leaf_finish(pieces, sums, beside)
    zorder = [m for m in range(blks - 4, 2, -2)] + [blks - 2, 2]
    got = [(m, exchange(s_all, 0, m)) for m in zorder]
    slot_other = exchange(slot_map, 0, 1)
    sep_rhs_other = exchange(sep_rhs, 0, 1)
    lower_other = exchange(leaf_lower, 0, 1)
    sep_lower_other = exchange(sep_lower, 0, 1)
    s_full = put(jnp.zeros((blks * rows, half), dtype), s_all, z)
    for m, value in got:
        s_full = put(s_full, value, z ^ (m // 2))

    inverse_others = [exchange(value, 0, 1) for value in inverse_rows]
    slots = in_order(slot_map, slot_other, 1)
    seps = in_order(columns_of(sep_rhs, core), columns_of(sep_rhs_other, core), 1)
    paired = levels > 1
    if paired:
        their_slots = exchange(slots[0], 1, 0)
        their_sep = exchange(seps[0], 1, 0)

    low_chip = in_order(sep_lower, sep_lower_other)
    inv_chip = in_order(sep_inverse[:, :top_offset], inverse_others[0][:, :top_offset])
    if paired:
        inv_own, inv_theirs = [
            in_order(mine[:, : 2 * base_width], other[:, : 2 * base_width])
            for mine, other in zip(inverse_rows[:2], inverse_others[:2])
        ]
        inv_pair = jnp.concatenate(
            [jnp.where(k % 2 == 1, inv_theirs, inv_own), jnp.where(k % 2 == 1, inv_own, inv_theirs)]
        )

    def top_columns(a, value):
        return leaf_columns(value, k) if a == 0 or send_whole else value[:, 2 * base_width :]

    top_blocks = []
    for a, (mine, other) in enumerate(zip(inverse_rows, inverse_others)):
        top_blocks.append(in_order(top_columns(a, mine), top_columns(a, other)))
    top_rows = jnp.concatenate(top_blocks[1:])

    lower_chip = in_order(leaf_lower, lower_other)
    update = -product(lower_chip, s_full)
    leaf_back = exchange(s_other, 0, 1)
    leaf_solution = in_order(s_mine, leaf_back, 1)

    def gather_z(piece):
        pieces = [piece] + [exchange(piece, 0, m) for m in range(blks - 2, 0, -2)]
        result = jnp.zeros((chips,) + piece.shape, piece.dtype)
        for m, value in zip([0] + list(range(chips - 1, 0, -1)), pieces):
            result = lax.dynamic_update_slice_in_dim(result, value[None], z ^ m, 0)
        return result

    def gather_node(piece, height):
        members = 2**height
        place = k % members
        if members * chips <= DIRECT_LIMIT:
            result = jnp.zeros((members * chips,) + piece.shape, piece.dtype)
            pieces = []
            for a in range(members):
                for m in range(chips):
                    value = piece if a == 0 and m == 0 else exchange(piece, a, 2 * m)
                    pieces.append(((place ^ a) * chips + (z ^ m), value))
            for where, value in pieces:
                result = lax.dynamic_update_slice_in_dim(result, value[None], where, 0)
            return result.reshape(-1, piece.shape[-1])
        joined = piece[None]
        for bit in range(height):
            theirs = exchange(joined, 2**bit, 0)
            upper = (k // 2**bit) % 2 == 1
            joined = jnp.concatenate(
                [jnp.where(upper, theirs, joined), jnp.where(upper, joined, theirs)], axis=0
            )
        return jnp.swapaxes(gather_z(joined), 0, 1).reshape(-1, piece.shape[-1])

    def mix(slot_rows, targets, count):
        result = []
        for t in count:
            hit = (targets == t)[:, :, None, None]
            result.append(jnp.sum(jnp.where(hit, slot_rows, 0), axis=1).reshape(-1, half))
        return result

    def rest_rows(front):
        slots_of = [value.reshape(2, pivots, half) for value in front]
        return jnp.stack(slots_of, axis=1).reshape(-1, half)

    solutions = []
    for height in range(1, levels):
        mask = 2 ** (height - 1)
        offset = base_width * (2**height - 2)
        width = base_width * 2**height
        targets = slots[height - 1]
        slot_rows = update.reshape(2, 2, pivots, half)
        theirs = exchange(slot_rows.astype(dtype), mask, 0).astype(jnp.float32)
        their_targets = their_slots if height == 1 else exchange(targets, mask, 0)
        own = mix(slot_rows, targets, range(3))
        sent = mix(theirs, their_targets, range(3, 6))
        pivot = (seps[height - 1].astype(jnp.float32) + own[0] + sent[0]).astype(dtype)
        rest = rest_rows([own[1] + sent[1], own[2] + sent[2]])
        inverse_here = inv_chip[:, offset : offset + width]
        if height == 1:
            upper = k % 2 == 1

            def by_leaf(near, far):
                return jnp.stack([jnp.where(upper, far, near), jnp.where(upper, near, far)])

            (their_own,) = mix(theirs, their_targets, range(1))
            (their_sent,) = mix(slot_rows, targets, range(3, 4))
            their_pivot = (their_sep.astype(jnp.float32) + their_own + their_sent).astype(dtype)
            pivots_all = gather_z(by_leaf(pivot, their_pivot))
            pivots_all = jnp.swapaxes(pivots_all, 0, 1).reshape(-1, half)
            both = product(inv_pair, pivots_all).astype(dtype)
            solved = lax.dynamic_slice_in_dim(both, k % 2 * 2 * pivots, 2 * pivots, 0)
            solved_all = gather_z(both.reshape(2, 2 * pivots, half))
            solved_all = jnp.swapaxes(solved_all, 0, 1).reshape(-1, half)
        else:
            solved = product(inverse_here, gather_node(pivot, height)).astype(dtype)
            solved_all = gather_node(solved, height)
        solutions.append(solved)
        update = rest - product(low_chip[:, offset : offset + width], solved_all)

    own, sent = mix(update.reshape(2, 2, pivots, half), slots[levels - 1], range(2))
    own = own + seps[levels - 1].astype(jnp.float32)
    parts = gather_z(jnp.stack([own, sent]).astype(dtype))
    contributions = jnp.swapaxes(parts, 0, 1).reshape(-1, half)
    sent_rows = product(top_rows, contributions)
    rounded = sent_rows.astype(dtype).reshape(leaves - 1, 2 * pivots, half)
    total = product(top_blocks[0], contributions)
    for a in range(leaves - 1, 0, -1):
        total = total + exchange(rounded[a - 1], a, 0).astype(jnp.float32)
    solutions.append(total.astype(dtype))

    outs = []
    for solved in solutions:
        mine = lax.dynamic_slice_in_dim(solved, core * pivots, pivots, 0)
        other = lax.dynamic_slice_in_dim(solved, (1 - core) * pivots, pivots, 0)
        outs.append(in_order(mine, exchange(other, 0, 1), 1))
    return leaf_solution, jnp.stack(outs)


def solution(mesh):
    return jax.shard_map(
        on_device,
        mesh=mesh,
        in_specs=(
            P(("leaf", "blk"), None),
            P(("leaf", "blk"), None),
            P(("leaf", "blk"), None),
            P(None, ("leaf", "blk"), None),
            P(("leaf", "blk"), None),
            P(("leaf", "blk"), None),
            P(None, ("leaf", "blk"), None),
        ),
        out_specs=(P(("leaf", "blk"), None), P(None, ("leaf", "blk"), None)),
        check_vma=False,
    )
```
